32 devices in a mesh: ma: 8 (over z, y), vert: 4 (over x, core).
Axes of the slice: x: 2, y: 2, z: 4, core: 2. Of those that a mesh axis runs over, the one named last changes fastest.
Arguments:
- trial_block: bfloat16 [128, 64, 4, 1024], P('vert', 'ma'), may hold values from -6 to 6
- legendre: bfloat16 [64, 2, 32, 1024], P('ma'), may hold values from -0.1875 to 0.1875
- order_slot: int32 [64], replicated, may hold values from 0 to 63, each once
- cycle_start: int32 [32], replicated, may hold values from 0 to 127
- cycle_count: int32 [32], replicated, may hold values from 0 to 128, as said below
- cycle_weight: float32 [32], replicated, may hold values from 4 to 32
Outputs:
- new_basis: bfloat16 [128, 64, 4, 1024], P('vert', 'ma')
- ritz_matrix: float32 [128, 128], replicated
The draws below stay inside these ranges and needn't reach their ends.
Inputs may be any that keep to these rules, and one draw needn't show every extreme that they name: `cycle_count`: exactly 8 consecutive cycles have a nonzero count, and one of them has 128.
All inputs are finite; a program needn't handle non-finite values.
Results may differ from the reference program's by a relative error of at most 0.0073.
The reference program's roundings to bfloat16 on the way (of `fields`, `weighted`, `returned`, `adjoint`, `applied` and `mixing`) count: a program that leaves them out, or rounds other values in their place, can miss the bound.
Values may be sent and summed in bfloat16 or wider, within the bound.
A program may use at most 192 MiB of HBM per device.

```python
import math
import jax
import jax.numpy as jnp
from jax import lax

LDEG = 1024
ORDERS = 64
CYCLES = 32
LIVE = 8
NLON = 128
K = 128
NC = 262144


def draw_cycle_count(key, part):
    keys = jax.random.split(jax.random.fold_in(key, 11), 3)
    band_start = jax.random.randint(keys[0], (), 0, CYCLES - LIVE + 1)
    counts = jax.random.randint(keys[1], (CYCLES,), 1, NLON + 1)
    full_cycle = jax.random.randint(keys[2], (), 0, LIVE)
    cycle_index = jnp.arange(CYCLES)
    inside = (cycle_index >= band_start) & (cycle_index < band_start + LIVE)
    counts = jnp.where(cycle_index == band_start + full_cycle, NLON, counts)
    return jnp.where(inside, counts, 0).astype(jnp.int32)


def set_ends(values, rng, smallest, high):
    index_at = [jax.random.randint(jax.random.fold_in(rng, axis), (), 0, length) for axis, length in enumerate(values.shape)]
    main_axis = values.shape.index(max(values.shape))
    next_to = index_at[:main_axis] + [(index_at[main_axis] + 1) % values.shape[main_axis]] + index_at[main_axis + 1:]
    return values.at[tuple(index_at)].set(smallest).at[tuple(next_to)].set(high)


def block_scale(key, shape, cuts, smallest, largest):
    loudness, own = 1.0, jax.random.fold_in(key, 6)
    for axis_at, parts in cuts:
        draws = jnp.exp(jax.random.uniform(jax.random.fold_in(own, axis_at), (parts,), jnp.float32, smallest / len(cuts), largest / len(cuts)))
        loudness = loudness * jnp.repeat(draws, shape[axis_at] // parts).reshape([-1 if axis == axis_at else 1 for axis in range(len(shape))])
    return loudness


def bell_draw(key, extent, width, limit, cuts=(), kind=jnp.bfloat16):
    array = width * jax.random.normal(key, extent, jnp.float32)
    if cuts:
        array = array * block_scale(key, extent, cuts, -0.22, 0.18)
    return jnp.clip(array, -limit, limit).astype(kind)


def setup_inputs(seed: int = 0) -> dict:
    key_list = jax.random.split(jax.random.key(seed), 7)
    return {
        "trial_block": bell_draw(key_list[0], (K, ORDERS, 4, LDEG), 1.0, 6.0, ((0, 4), (1, 8))),
        "legendre": bell_draw(key_list[1], (ORDERS, 2, CYCLES, LDEG), LDEG ** -0.5, 0.1875, ((0, 8),)),
        "order_slot": jax.random.permutation(key_list[2], ORDERS).astype(jnp.int32),
        "cycle_start": set_ends(jax.random.randint(key_list[3], (CYCLES,), 0, NLON), jax.random.fold_in(key_list[3], 1), 0, NLON - 1).astype(jnp.int32),
        "cycle_count": draw_cycle_count(jax.random.fold_in(key_list[6], 71), 0),
        "cycle_weight": jnp.clip(jnp.exp(jax.random.uniform(key_list[5], (CYCLES,), jnp.float32, math.log(4.0), math.log(32.0))), 4.0, 32.0),
    }


def combine_fields(products):
    first_kind = products[:, 0]
    second_kind = products[:, 1]
    return jnp.stack([first_kind[..., 0] + second_kind[..., 3], first_kind[..., 1] - second_kind[..., 2], second_kind[..., 1] - first_kind[..., 2], -second_kind[..., 0] - first_kind[..., 3]], axis=-1)

def adjoint_terms(returned):
    gtc = returned[..., 0]
    gts = returned[..., 1]
    gpc = returned[..., 2]
    gps = returned[..., 3]
    first_kind = jnp.stack([gtc, gts, -gpc, -gps], axis=-1)
    second_kind = jnp.stack([-gps, gpc, -gts, gtc], axis=-1)
    return jnp.stack([first_kind, second_kind], axis=1)

def fourier_tables(order_slot, longitudes, orders_total):
    longitude = jnp.arange(longitudes, dtype=jnp.int32)
    phases = longitude[:, None] * order_slot[None, :].astype(jnp.int32) % longitudes
    angles = phases.astype(jnp.float32) * (2.0 * math.pi / longitudes)
    scale = 1.0 / math.sqrt(orders_total)
    return ((jnp.cos(angles) * scale).astype(jnp.bfloat16), (jnp.sin(angles) * scale).astype(jnp.bfloat16))

def finish_ritz(gram_trial, cross, gram_applied):
    factor_trial = jnp.linalg.cholesky(gram_trial)
    half_solved = lax.linalg.triangular_solve(factor_trial, cross, left_side=True, lower=True)
    ritz_matrix = lax.linalg.triangular_solve(factor_trial, half_solved.T, left_side=True, lower=True).T
    factor_applied = jnp.linalg.cholesky(gram_applied)
    identity = jnp.eye(gram_applied.shape[0], dtype=gram_applied.dtype)
    mixing = lax.linalg.triangular_solve(factor_applied, identity, left_side=True, lower=True)
    return (ritz_matrix, mixing.astype(jnp.bfloat16))

def reference(trial_block, legendre, order_slot, cycle_start, cycle_count, cycle_weight):
    highest = lax.Precision.HIGHEST
    block = trial_block.astype(jnp.float32)
    table = legendre.astype(jnp.float32)
    products = lax.dot_general(table, block, (((3,), (3,)), ((0,), (1,))), precision=highest)
    fields = combine_fields(products).astype(jnp.bfloat16)
    cosine, sines = fourier_tables(order_slot, NLON, ORDERS)
    cosine_wide = cosine.astype(jnp.float32)
    sines_wide = sines.astype(jnp.float32)
    pieces = fields.astype(jnp.float32)
    grid_values = jnp.einsum('jo,orkc->rckj', cosine_wide, pieces[..., 0::2], precision=highest)
    grid_values = grid_values + jnp.einsum('jo,orkc->rckj', sines_wide, pieces[..., 1::2], precision=highest)
    longitude = jnp.arange(NLON, dtype=jnp.int32)
    inside = ((longitude[None, :] - cycle_start[:, None]) % NLON < cycle_count[:, None]).astype(jnp.float32)
    factor = inside * cycle_weight[:, None].astype(jnp.float32)
    weighted = (grid_values * factor[:, None, None, :]).astype(jnp.bfloat16).astype(jnp.float32)
    back_cos = jnp.einsum('jo,rckj->orkc', cosine_wide, weighted, precision=highest)
    back_sin = jnp.einsum('jo,rckj->orkc', sines_wide, weighted, precision=highest)
    returned = jnp.stack([back_cos[..., 0], back_sin[..., 0], back_cos[..., 1], back_sin[..., 1]], axis=-1).astype(jnp.bfloat16)
    adjoint = adjoint_terms(returned).astype(jnp.float32)
    adjoint = adjoint.reshape(ORDERS, 2, CYCLES, K * 4)
    applied = lax.dot_general(adjoint, table, (((1, 2), (1, 2)), ((0,), (0,))), precision=highest)
    applied = applied.reshape(ORDERS, K, 4, LDEG).transpose(1, 0, 2, 3).astype(jnp.bfloat16)
    trial_flat = trial_block.reshape(K, NC)
    applied_flat = applied.reshape(K, NC)
    gram_trial = jnp.dot(trial_flat.astype(jnp.float32), trial_flat.T.astype(jnp.float32), preferred_element_type=jnp.float32) / NC
    cross = jnp.dot(trial_flat.astype(jnp.float32), applied_flat.T.astype(jnp.float32), preferred_element_type=jnp.float32) / NC
    gram_applied = jnp.dot(applied_flat.astype(jnp.float32), applied_flat.T.astype(jnp.float32), preferred_element_type=jnp.float32) / NC
    ritz_matrix, mixing = finish_ritz(gram_trial, cross, gram_applied)
    new_basis = jnp.dot(mixing.astype(jnp.float32), applied_flat.astype(jnp.float32), preferred_element_type=jnp.float32)
    new_basis = new_basis.reshape(K, ORDERS, 4, LDEG).astype(jnp.bfloat16)
    return (new_basis, ritz_matrix)
```

```python
import functools
import math

import jax
import jax.numpy as jnp
from jax import lax
from jax.experimental import pallas as pl
from jax.experimental.pallas import tpu as pltpu
from jax.sharding import PartitionSpec as P

MESH = pl.DeviceIdType.MESH
VMEM = pltpu.VMEM
SMEM = pltpu.SMEM
DMA = pltpu.SemaphoreType.DMA
F32 = jnp.float32
BF16 = jnp.bfloat16
I32 = jnp.int32
HIGHEST = lax.Precision.HIGHEST
GRANT = 60 * 1024 * 1024
LANES = 128
PANEL = 16
NT = (((1,), (1,)), ((), ()))
STAGES = (7, 12)


def iota(shape, axis):
    return lax.broadcasted_iota(I32, shape, axis)


def mm(a, b):
    return jnp.dot(a, b, preferred_element_type=F32)


def mm_nt(a, b):
    return lax.dot_general(a, b, NT, preferred_element_type=F32)


def split(x, count):
    pieces = []
    for _ in range(count):
        piece = x.astype(BF16)
        pieces.append(piece)
        x = x - piece.astype(F32)
    return pieces


def swap(x):
    return pltpu.roll(x, x.shape[1] // 2, 1)


def half_sign(shape, first, second):
    return jnp.where(iota(shape, 1) < shape[1] // 2, first, second).astype(F32)


def rows_at(index, count):
    return pl.ds(pl.multiple_of(index * count, count), count)


def factor_panel(work, p):
    size = work.shape[0]
    first = pl.multiple_of(p * PANEL, PANEL)
    at = pl.ds(first, PANEL)
    lane = iota((PANEL, size), 1)
    sub = iota((PANEL, 2 * size), 0)
    x = work[at, :]
    column = [
        jnp.sum(jnp.where(lane == first + i, x[:, :size], 0.0), axis=1, keepdims=True)
        for i in range(PANEL)
    ]
    for i in range(PANEL):
        inverse = lax.rsqrt(column[i][i : i + 1, :])
        scaled = column[i] * inverse
        for k in range(i + 1, PANEL):
            column[k] = column[k] - scaled * (column[k][i : i + 1, :] * inverse)
        line = x[i : i + 1, :] * inverse
        x = jnp.where(sub == i, line, jnp.where(sub > i, x - scaled * line, x))
    update = lax.dot_general(
        x[:, :size], x, (((0,), (0,)), ((), ())),
        precision=HIGHEST, preferred_element_type=F32,
    )
    below = iota((size, 2 * size), 0) >= first + PANEL
    work[...] = jnp.where(below, work[...] - update, work[...])
    work[at, :] = x


def cosines(phase, total):
    phase = jnp.where(phase > total // 2, total - phase, phase)
    turned = phase > total // 4
    x = jnp.where(turned, total // 2 - phase, phase).astype(F32) * (2.0 * math.pi / total)
    y = x * x
    value = jnp.full_like(y, 1.0 / math.factorial(12))
    for n in (10, 8, 6, 4, 2, 0):
        value = value * y * (1.0 if n % 4 == 2 else 1.0) + (-1.0) ** (n // 2) / math.factorial(n)
    return jnp.where(turned, -value, value)


def modulo(x, total):
    return x & (total - 1) if total & (total - 1) == 0 else lax.rem(x, total)


def step_kernel(
    n_ma, n_vert, live,
    trial_ref, legendre_ref, order_ref, start_ref, count_ref, weight_ref,
    rows_ref, ab_ref, mixer_ref, leg_ref,
    native, leg_in, near, far, message, gathered, spectra, returned, packed,
    row_a, land_a, sum_a, row_b, land_b, ab_own, land_c, ab_mid, land_d,
    work, lhs, llm, tables, back_table,
    load_sem, leg_sem, near_send, near_recv, far_send, far_recv,
    ma_send, ma_recv, vert_send, vert_recv,
):
    ma = lax.axis_index("ma")
    vert = lax.axis_index("vert")
    pairs, vectors, _, per, _ = native.shape
    orders = 2 * pairs
    parts, degrees = near.shape[2], near.shape[4]
    tiles = degrees // LANES
    cycles = leg_in.shape[2]
    half = n_vert // 2
    share = orders // n_vert
    place = lax.rem(vert, half)
    side = vert // half
    total = n_vert * vectors
    terms = live * orders
    longitudes = 2 * n_ma * orders

    barrier = pltpu.get_barrier_semaphore()

    def ma_peer(step):
        return lax.rem(ma + step, n_ma)

    def vert_peer(step):
        return lax.rem(vert + step, n_vert)

    def greet_ma(step, carry):
        pl.semaphore_signal(barrier, inc=1, device_id=(ma_peer(step), vert), device_id_type=MESH)
        return carry

    def greet_vert(step, carry):
        pl.semaphore_signal(barrier, inc=1, device_id=(ma, vert_peer(step)), device_id_type=MESH)
        return carry

    lax.fori_loop(1, n_ma, greet_ma, 0)
    lax.fori_loop(1, n_vert, greet_vert, 0)

    def load(pair):
        at = pl.ds(2 * pair, 2)
        return pltpu.make_async_copy(trial_ref.at[:, at], native.at[pair], load_sem.at[pair])

    def pair_at(i):
        return lax.rem((1 - side) * (orders // 4) + i, orders // 2)

    for i in range(orders // 2):
        load(pair_at(i)).start()
    leg_copy = pltpu.make_async_copy(legendre_ref, leg_in, leg_sem)
    leg_copy.start()

    rows = 8 * per
    row = iota((rows, rows), 0)
    column = iota((rows, rows), 1)
    wanted = lax.rem(row, 8) * per + lax.rem(row // 8, tiles) * parts + row // (8 * tiles)
    reorder = (column == wanted).astype(BF16)

    for i in range(orders // 2):
        load(pair_at(i)).wait()
    leg_copy.wait()

    def arrange(i, carry):
        pair = pair_at(i)
        for g in range(vectors // 16):
            blocks = []
            for h in range(2):
                at = pl.ds(16 * g + 8 * h, 8)
                both = [native[pair, at, e].reshape(rows, LANES) for e in range(2)]
                blocks.append(mm(reorder, jnp.concatenate(both, axis=1)))
            for e in range(2):
                for c in range(parts):
                    for t in range(tiles):
                        lo = (c * tiles + t) * 8
                        at = (slice(lo, lo + 8), slice(e * LANES, (e + 1) * LANES))
                        tile = jnp.concatenate([blocks[0][at], blocks[1][at]], axis=0)
                        at = (slice(16 * g, 16 * g + 16), slice(t * LANES, (t + 1) * LANES))
                        near[(place, 2 * pair + e, c) + at] = tile.astype(BF16)
        return carry

    lax.fori_loop(0, orders // 2, arrange, 0)

    def search(i, found):
        j = cycles - 1 - i
        return jnp.where(count_ref[j] > 0, j, found)

    first = jnp.minimum(lax.fori_loop(0, cycles, search, 0), cycles - live)

    block = min(terms, 64)
    for kind in range(2):
        source = leg_in[:, kind].reshape(orders * cycles, degrees)

        def pick(i, carry):
            row = iota((block, orders * cycles), 0) + i * block
            column = iota((block, orders * cycles), 1)
            wanted = lax.rem(row, orders) * cycles + row // orders + first
            at = rows_at(kind * (terms // block) + i, block)
            leg_ref[at, :] = mm((column == wanted).astype(BF16), source).astype(BF16)
            return carry

        lax.fori_loop(0, terms // block, pick, 0)

    pl.semaphore_wait(barrier, n_ma + n_vert - 2)

    def near_copy(peer, slot, source):
        return pltpu.make_async_remote_copy(
            src_ref=near.at[source],
            dst_ref=near.at[source],
            send_sem=near_send.at[slot],
            recv_sem=near_recv.at[slot],
            device_id=(ma, peer),
            device_id_type=MESH,
        )

    pieces = half * share * parts

    def far_copy(piece, arriving=False):
        offset = lax.rem(piece, half)
        inner = piece // half
        peer = (1 - side) * half + lax.rem(place + offset, half)
        slot = lax.rem(place + half - offset, half) if arriving else place
        s = inner // parts
        c = lax.rem(inner, parts)
        return pltpu.make_async_remote_copy(
            src_ref=near.at[slot, peer * share + s, c],
            dst_ref=far.at[slot, s, c],
            send_sem=far_send.at[piece],
            recv_sem=far_recv.at[piece],
            device_id=(ma, peer),
            device_id_type=MESH,
        )

    def send_far(begin, end):
        def body(piece, carry):
            far_copy(piece).start()
            return carry

        lax.fori_loop(begin, end, body, 0)

    cuts = [min(pieces, cut) for cut in STAGES]
    send_far(0, cuts[0])
    for step in range(1, half):
        near_copy(side * half + lax.rem(place + step, half), step, place).start()

    keep = lax.rem(iota((2 * terms, LANES), 0), orders)

    def product(s, carry):
        vectors_here = near[place, s].reshape(parts * vectors, degrees)
        found = mm_nt(leg_ref[...], vectors_here)
        spectra[...] = jnp.where(keep == s, found, spectra[...])
        return carry

    lax.fori_loop(0, orders, product, 0)
    w = spectra[:terms, :]
    x = spectra[terms:, :]
    quarter = iota((terms, LANES), 1) // vectors
    left = lambda a: pltpu.roll(a, LANES - vectors, 1)
    right = lambda a: pltpu.roll(a, vectors, 1)
    w = jnp.where(quarter == 1, left(w), jnp.where(quarter == 2, right(w), w))
    x = jnp.where(quarter == 0, right(x), jnp.where(quarter == 3, left(x), x))
    w = jnp.where((quarter == 1) | (quarter == 3), -w, w)
    fields = w + jnp.where(quarter >= 2, -x, x)
    front = iota((orders, LANES), 1) < LANES // 2
    for pair in range(live // 2):
        a = fields[2 * pair * orders : (2 * pair + 1) * orders]
        b = fields[(2 * pair + 1) * orders : (2 * pair + 2) * orders]
        both = jnp.concatenate([jnp.where(front, a, swap(b)), jnp.where(front, swap(a), b)], axis=0)
        message[:, pair * LANES : (pair + 1) * LANES] = both.astype(BF16)

    def ma_copy(kind, source, target, slot, peer):
        return pltpu.make_async_remote_copy(
            src_ref=source,
            dst_ref=target.at[slot],
            send_sem=ma_send.at[kind, peer],
            recv_sem=ma_recv.at[kind, slot],
            device_id=(peer, vert),
            device_id_type=MESH,
        )

    def over_ma(act):
        def body(step, carry):
            act(ma_peer(step))
            return carry

        lax.fori_loop(1, n_ma, body, 0)

    def ma_start(kind, source, target):
        over_ma(lambda peer: ma_copy(kind, source, target, ma, peer).start())

    def ma_wait(kind, source, target):
        over_ma(lambda peer: ma_copy(kind, source, target, peer, peer).wait_recv())

    def ma_done(kind, source, target):
        over_ma(lambda peer: ma_copy(kind, source, target, ma, peer).wait_send())

    def vert_copy(kind, source, target, slot, peer):
        return pltpu.make_async_remote_copy(
            src_ref=source,
            dst_ref=target.at[slot],
            send_sem=vert_send.at[kind, peer],
            recv_sem=vert_recv.at[kind, slot],
            device_id=(ma, peer),
            device_id_type=MESH,
        )

    def over_vert(act):
        def body(step, carry):
            act(vert_peer(step))
            return carry

        lax.fori_loop(1, n_vert, body, 0)

    def vert_start(kind, source, target):
        over_vert(lambda peer: vert_copy(kind, source, target, vert, peer).start())

    def vert_wait(kind, source, target):
        over_vert(lambda peer: vert_copy(kind, source, target, peer, peer).wait_recv())

    def vert_done(kind, source, target):
        over_vert(lambda peer: vert_copy(kind, source, target, vert, peer).wait_send())

    ma_start(0, message, gathered)
    gathered[ma] = message[...]

    turned = spectra[...].T
    part = [turned[c * vectors : (c + 1) * vectors] for c in range(parts)]
    wide = part[0].shape
    sign = half_sign(wide, 1.0, -1.0)
    field_x = (part[0] + swap(part[3])) * sign
    field_y = part[1] - swap(part[2])
    for n, (piece_x, piece_y) in enumerate(zip(split(field_x, 3), split(field_y, 3))):
        at = slice((3 + n) * vectors, (4 + n) * vectors)
        lhs[at, : 2 * terms] = piece_x
        lhs[at, 2 * terms :] = piece_y

    step_rows = min(2 * terms, LANES)

    def leg_products(i, carry):
        at = rows_at(i, step_rows)
        found = mm_nt(leg_ref[at, :], leg_ref[...])
        same = lax.rem(iota(found.shape, 0) - iota(found.shape, 1) + 2 * terms * orders, orders) == 0
        for n, piece in enumerate(split(jnp.where(same, found, 0.0), 3)):
            llm[n, at, :] = piece
        return carry

    lax.fori_loop(0, 2 * terms // step_rows, leg_products, 0)

    scale = 1.0 / math.sqrt(n_ma * orders)
    width = n_ma * 2 * orders
    lane = iota((8, width), 1)
    slot = lane // (2 * orders) * orders + lax.rem(lane, orders)

    def place_order(i, carry):
        return jnp.where(slot == i, order_ref[i], carry)

    lane_order = lax.fori_loop(0, n_ma * orders, place_order, jnp.zeros((8, width), I32))
    shift = jnp.where(lax.rem(lane // orders, 2) == 1, longitudes - longitudes // 4, 0)

    def table_rows(i, carry):
        j = iota((LANES, width), 0) + i * LANES
        phase = modulo(j * lane_order[:1] + shift[:1], longitudes)
        tables[rows_at(i, LANES), :] = (cosines(phase, longitudes) * scale).astype(BF16)
        return carry

    lax.fori_loop(0, longitudes // LANES, table_rows, 0)
    row = iota((2 * orders, longitudes), 0)
    own_order = jnp.zeros((2 * orders, longitudes), I32)
    for s in range(orders):
        own_order = jnp.where(lax.rem(row, orders) == s, order_ref[ma * orders + s], own_order)
    phase = iota((2 * orders, longitudes), 1) * own_order
    phase = phase + jnp.where(row >= orders, longitudes - longitudes // 4, 0)
    back_table[...] = (cosines(modulo(phase, longitudes), longitudes) * scale).astype(BF16)

    for step in range(1, half):
        peer = side * half + lax.rem(place + step, half)
        near_copy(peer, half - step, lax.rem(place + step, half)).wait_recv()

    def near_gram(s, sums):
        for c in range(parts):
            sums = sums + mm_nt(near[place, s, c], near[:, s, c].reshape(half * vectors, degrees))
        return sums

    near_sums = lax.fori_loop(0, orders, near_gram, jnp.zeros((vectors, half * vectors), F32))
    row_b[:, total:] = jnp.concatenate([near_sums, jnp.zeros_like(near_sums)], axis=1)

    ma_wait(0, message, gathered)
    columns = message.shape[1]
    wide_block = min(columns, 512)
    cycles_here = wide_block // (2 * vectors)

    def transform(block, carry):
        at = rows_at(block, wide_block)
        grid = mm(tables[...], gathered[:, :, at].reshape(n_ma * 2 * orders, wide_block))
        lane_cycle = iota((8, wide_block), 1) // (2 * vectors)
        begin = jnp.zeros((8, wide_block), I32)
        length = jnp.zeros((8, wide_block), I32)
        weight = jnp.zeros((8, wide_block), F32)
        for r in range(cycles_here):
            here = lane_cycle == r
            cycle = first + block * cycles_here + r
            begin = jnp.where(here, start_ref[cycle], begin)
            length = jnp.where(here, count_ref[cycle], length)
            weight = jnp.where(here, weight_ref[cycle], weight)
        away = iota(grid.shape, 0) - begin[:1]
        away = jnp.where(away < 0, away + longitudes, away)
        weighted = (grid * jnp.where(away < length[:1], weight[:1], 0.0)).astype(BF16)
        found = mm(back_table[...], weighted)
        for n in range(wide_block // LANES):
            both = found[:, n * LANES : (n + 1) * LANES]
            c, s = both[:orders], both[orders:]
            pair = [jnp.where(front, c, swap(s)), jnp.where(front, swap(c), s)]
            for e in range(2):
                cycle = block * cycles_here + 2 * n + e
                returned[rows_at(cycle, orders), :] = pair[e]
        return carry

    lax.fori_loop(0, columns // wide_block, transform, 0)
    here = returned[...]
    even = lax.rem(iota(here.shape, 1) // vectors, 2) == 0
    turned = jnp.concatenate([here, jnp.where(even, right(here), left(here))], axis=0).T
    turned = turned.astype(BF16)
    g_x = turned[:vectors]
    back_y = turned[vectors : 2 * vectors]
    g_y = turned[2 * vectors : 3 * vectors]
    back_x = turned[3 * vectors :]
    packed[vert, :, : 2 * terms] = g_x
    packed[vert, :, 2 * terms :] = g_y
    vert_start(0, packed.at[vert], packed)
    send_far(cuts[0], cuts[1])

    signs = sign.astype(BF16)
    adjoint = jnp.concatenate([g_x * signs, g_y, -back_y, -back_x * signs], axis=0)
    products = mm(adjoint, llm[0]) + mm(adjoint, llm[1]) + mm(adjoint, llm[2])
    part = [products[c * vectors : (c + 1) * vectors] for c in range(parts)]
    gram_x = part[0] * sign + swap(part[3] * -sign)
    gram_y = part[1] - swap(part[2])
    for n, (piece_x, piece_y) in enumerate(zip(split(gram_x, 3), split(gram_y, 3))):
        at = slice(n * vectors, (n + 1) * vectors)
        lhs[at, : 2 * terms] = piece_x
        lhs[at, 2 * terms :] = piece_y

    vert_wait(0, packed.at[vert], packed)
    everyone = packed[...].reshape(total, 4 * terms)
    found = mm_nt(lhs[...], everyone)
    found = [found[n * vectors : (n + 1) * vectors] for n in range(6)]
    row_a[...] = found[0] + found[1] + found[2]
    ma_start(1, row_a, land_a)
    land_a[ma] = row_a[...]
    row_b[:, :total] = found[3] + found[4] + found[5]
    ma_start(2, row_b, land_b)
    land_b[ma] = row_b[...]
    ma_wait(1, row_a, land_a)
    sum_a[vert] = jnp.sum(land_a[...], axis=0)
    vert_start(1, sum_a.at[vert], sum_a)
    ma_wait(2, row_b, land_b)
    rows_ref[vert] = jnp.sum(land_b[...], axis=0)
    vert_start(2, rows_ref.at[vert], rows_ref)
    send_far(cuts[1], pieces)

    vert_wait(1, sum_a.at[vert], sum_a)
    inverse_count = 1.0 / (n_ma * orders * parts * degrees)
    work[:, :total] = sum_a[...].reshape(total, total) * inverse_count
    work[:, total:] = (iota((total, total), 0) == iota((total, total), 1)).astype(F32)

    def panel_step(p, carry):
        factor_panel(work, p)
        return carry

    panels = total // PANEL
    lax.fori_loop(0, panels // 2, panel_step, 0)

    def far_wait(piece, carry):
        far_copy(piece, True).wait_recv()
        return carry

    lax.fori_loop(0, pieces, far_wait, 0)

    def far_gram(s, sums):
        for c in range(parts):
            here = near[:, vert * share + s, c].reshape(half * vectors, degrees)
            sums = sums + mm_nt(here, far[:, s, c].reshape(half * vectors, degrees))
        return sums

    cross_sums = lax.fori_loop(
        0, share, far_gram, jnp.zeros((half * vectors, half * vectors), F32)
    )
    cross_sums = jnp.where(side == 0, cross_sums, cross_sums.T)
    size = half * vectors
    ab_own[...] = jnp.concatenate([cross_sums[: size // 2], cross_sums[size // 2 :]], axis=1)
    vert_start(3, ab_own, land_c)
    land_c[vert] = ab_own[...]
    lax.fori_loop(panels // 2, panels, panel_step, 0)
    vert_wait(3, ab_own, land_c)
    ab_mid[...] = jnp.sum(land_c[...], axis=0)
    ma_start(3, ab_mid, land_d)
    land_d[ma] = ab_mid[...]

    mixing = work[rows_at(vert, vectors), total:].astype(BF16)
    spread = (iota((parts * vectors, vectors), 0) // parts == iota((parts * vectors, vectors), 1))
    mixing = mm(spread.astype(BF16), mixing).astype(BF16)
    mixed = mm(mixing, everyone)
    mixed_x, mixed_y = mixed[:, : 2 * terms], mixed[:, 2 * terms :]
    kind = lax.rem(iota(mixed_x.shape, 0), parts)
    sign = half_sign(mixed_x.shape, 1.0, -1.0)
    mixer = jnp.where(
        kind == 0, mixed_x * sign,
        jnp.where(kind == 1, mixed_y, jnp.where(kind == 2, -swap(mixed_y), -swap(mixed_x) * sign)),
    )
    high, low = split(mixer, 2)
    mixer_ref[:, : 2 * terms] = high
    mixer_ref[:, 2 * terms :] = low

    vert_wait(2, rows_ref.at[vert], rows_ref)
    ma_wait(3, ab_mid, land_d)
    ab_ref[...] = jnp.sum(land_d[...], axis=0)

    for step in range(1, half):
        near_copy(side * half + lax.rem(place + step, half), step, place).wait_send()

    def far_done(piece, carry):
        far_copy(piece).wait_send()
        return carry

    lax.fori_loop(0, pieces, far_done, 0)
    ma_done(0, message, gathered)
    vert_done(0, packed.at[vert], packed)
    ma_done(1, row_a, land_a)
    ma_done(2, row_b, land_b)
    vert_done(1, sum_a.at[vert], sum_a)
    vert_done(2, rows_ref.at[vert], rows_ref)
    vert_done(3, ab_own, land_c)
    ma_done(3, ab_mid, land_d)


def step_terms(trial, legendre, order_slot, cycle_start, cycle_count, cycle_weight, n_ma, n_vert):
    vectors, orders, per, _ = trial.shape
    _, kinds, cycles, degrees = legendre.shape
    parts = per * LANES // degrees
    live = cycles // 4
    terms = live * orders
    total = n_vert * vectors
    half = n_vert // 2
    share = orders // n_vert
    longitudes = 2 * n_ma * orders
    pieces = half * share * parts
    columns = live * 2 * vectors
    anywhere = pl.BlockSpec(memory_space=pl.ANY)
    return pl.pallas_call(
        functools.partial(step_kernel, n_ma, n_vert, live),
        out_shape=(
            jax.ShapeDtypeStruct((n_vert, vectors, total + 2 * half * vectors), F32),
            jax.ShapeDtypeStruct((half * vectors // 2, 2 * half * vectors), F32),
            jax.ShapeDtypeStruct((parts * vectors, 4 * terms), BF16),
            jax.ShapeDtypeStruct((2 * terms, degrees), BF16),
        ),
        in_specs=[anywhere, anywhere] + [pl.BlockSpec(memory_space=SMEM)] * 4,
        out_specs=[pl.BlockSpec(memory_space=VMEM)] * 4,
        scratch_shapes=[
            VMEM((orders // 2, vectors, 2, per, LANES), BF16),
            VMEM(legendre.shape, BF16),
            VMEM((half, orders, parts, vectors, degrees), BF16),
            VMEM((half, share, parts, vectors, degrees), BF16),
            VMEM((2 * orders, columns), BF16),
            VMEM((n_ma, 2 * orders, columns), BF16),
            VMEM((2 * terms, LANES), F32),
            VMEM((terms, LANES), F32),
            VMEM((n_vert, vectors, 4 * terms), BF16),
            VMEM((vectors, total), F32),
            VMEM((n_ma, vectors, total), F32),
            VMEM((n_vert, vectors, total), F32),
            VMEM((vectors, total + 2 * half * vectors), F32),
            VMEM((n_ma, vectors, total + 2 * half * vectors), F32),
            VMEM((half * vectors // 2, 2 * half * vectors), F32),
            VMEM((n_vert, half * vectors // 2, 2 * half * vectors), F32),
            VMEM((half * vectors // 2, 2 * half * vectors), F32),
            VMEM((n_ma, half * vectors // 2, 2 * half * vectors), F32),
            VMEM((total, 2 * total), F32),
            VMEM((6 * vectors, 4 * terms), BF16),
            VMEM((3, 2 * terms, 2 * terms), BF16),
            VMEM((longitudes, n_ma * 2 * orders), BF16),
            VMEM((2 * orders, longitudes), BF16),
            DMA((orders // 2,)),
            DMA,
            DMA((half,)),
            DMA((half,)),
            DMA((pieces,)),
            DMA((pieces,)),
            DMA((4, n_ma)),
            DMA((4, n_ma)),
            DMA((4, n_vert)),
            DMA((4, n_vert)),
        ],
        compiler_params=pltpu.CompilerParams(
            collective_id=0, has_side_effects=True, vmem_limit_bytes=GRANT
        ),
        name="step_terms",
    )(trial, legendre, order_slot, cycle_start, cycle_count, cycle_weight)


def finish_kernel(
    coefficients, rows_ref, ab_ref, mixer_ref, leg_ref, basis_ref, ritz_ref, work, staged, sems
):
    total = ritz_ref.shape[0]
    size = total // 2
    orders, vectors, parts, degrees = staged.shape
    scale = 1.0 / coefficients
    own = rows_ref[...].reshape(total, rows_ref.shape[2])
    ab = ab_ref[...]
    ab = jnp.concatenate([ab[:, :size], ab[:, size:]], axis=0)
    top = jnp.concatenate([own[:size, total : total + size], ab], axis=1)
    bottom = jnp.concatenate([ab.T, own[size:, total : total + size]], axis=1)
    work[:, :total] = jnp.concatenate([top, bottom], axis=0) * scale
    work[:, total:] = (iota((total, total), 0) == iota((total, total), 1)).astype(F32)
    mixer = mixer_ref[...]
    lane_order = lax.rem(iota(mixer.shape, 1), orders)

    def out_copy(s):
        return pltpu.make_async_copy(staged.at[s], basis_ref.at[:, s], sems.at[s])

    def mix(s):
        picked = jnp.where(lane_order == s, mixer, jnp.zeros_like(mixer))
        width = mixer.shape[1] // 2
        mixed = mm(picked[:, :width], leg_ref[...]) + mm(picked[:, width:], leg_ref[...])
        staged[s] = mixed.reshape(vectors, parts, degrees).astype(BF16)
        out_copy(s).start()

    panels = total // PANEL
    assert panels == orders

    def step(p, carry):
        factor_panel(work, p)
        mix(p)
        return carry

    lax.fori_loop(0, panels, step, 0)
    inverse = work[:, total:]
    half = jnp.dot(inverse, own[:, :total] * scale, precision=HIGHEST, preferred_element_type=F32)
    ritz_ref[...] = lax.dot_general(
        half, inverse, NT, precision=HIGHEST, preferred_element_type=F32
    )

    def done(s, carry):
        out_copy(s).wait()
        return carry

    lax.fori_loop(0, orders, done, 0)


def finish(rows, ab, mixer, table, vectors, orders, coefficients):
    total = rows.shape[0] * rows.shape[1]
    degrees = table.shape[1]
    parts = mixer.shape[0] // vectors
    return pl.pallas_call(
        functools.partial(finish_kernel, float(coefficients)),
        out_shape=(
            jax.ShapeDtypeStruct((vectors, orders, parts, degrees), BF16),
            jax.ShapeDtypeStruct((total, total), F32),
        ),
        in_specs=[pl.BlockSpec(memory_space=VMEM)] * 4,
        out_specs=(pl.BlockSpec(memory_space=pl.ANY), pl.BlockSpec(memory_space=VMEM)),
        scratch_shapes=[
            VMEM((total, 2 * total), F32),
            VMEM((orders, vectors, parts, degrees), BF16),
            DMA((orders,)),
        ],
        compiler_params=pltpu.CompilerParams(vmem_limit_bytes=32 * 1024 * 1024),
        name="finish",
    )(rows, ab, mixer, table)


def shards(trial_block, legendre, order_slot, cycle_start, cycle_count, cycle_weight):
    n_ma = lax.axis_size("ma")
    n_vert = lax.axis_size("vert")
    vectors, orders, parts, degrees = trial_block.shape
    trial = trial_block.reshape(vectors, orders, parts, degrees // LANES, LANES)
    trial = trial.transpose(0, 1, 3, 2, 4).reshape(vectors, orders, parts * degrees // LANES, LANES)
    terms = step_terms(
        trial, legendre, order_slot, cycle_start, cycle_count, cycle_weight, n_ma, n_vert
    )
    coefficients = order_slot.shape[0] * parts * degrees
    return finish(*terms, vectors, orders, coefficients)


def solution(mesh):
    in_specs = (P("vert", "ma", None, None), P("ma", None, None, None), P(), P(), P(), P())
    out_specs = (P("vert", "ma", None, None), P())
    return jax.shard_map(shards, mesh=mesh, in_specs=in_specs, out_specs=out_specs, check_vma=False)
```

```python
import functools
import math

import jax
import jax.numpy as jnp
from jax import lax
from jax.experimental import pallas as pl
from jax.experimental.pallas import tpu as pltpu
from jax.sharding import PartitionSpec as P

MESH = pl.DeviceIdType.MESH
VMEM = pltpu.VMEM
SMEM = pltpu.SMEM
DMA = pltpu.SemaphoreType.DMA
F32 = jnp.float32
BF16 = jnp.bfloat16
I32 = jnp.int32
HIGHEST = lax.Precision.HIGHEST
MIB = 1024 * 1024
LANES = 128
PANEL = 16
NT = (((1,), (1,)), ((), ()))
STAGES = (7, 13)


def iota(shape, axis):
    return lax.broadcasted_iota(I32, shape, axis)


def mm(a, b):
    return jnp.dot(a, b, preferred_element_type=F32)


def mm_nt(a, b):
    return lax.dot_general(a, b, NT, preferred_element_type=F32)


def split(x, count):
    pieces = []
    for _ in range(count):
        piece = x.astype(BF16)
        pieces.append(piece)
        x = x - piece.astype(F32)
    return pieces


def swap(x):
    return pltpu.roll(x, x.shape[1] // 2, 1)


def half_sign(shape, first, second):
    return jnp.where(iota(shape, 1) < shape[1] // 2, first, second).astype(F32)


def rows_at(index, count):
    return pl.ds(pl.multiple_of(index * count, count), count)


def factor_panel(work, p):
    size = work.shape[0]
    first = pl.multiple_of(p * PANEL, PANEL)
    at = pl.ds(first, PANEL)
    lane = iota((PANEL, size), 1)
    sub = iota((PANEL, 2 * size), 0)
    x = work[at, :]
    column = [
        jnp.sum(jnp.where(lane == first + i, x[:, :size], 0.0), axis=1, keepdims=True)
        for i in range(PANEL)
    ]
    for i in range(PANEL):
        inverse = lax.rsqrt(column[i][i : i + 1, :])
        scaled = column[i] * inverse
        for k in range(i + 1, PANEL):
            column[k] = column[k] - scaled * (column[k][i : i + 1, :] * inverse)
        line = x[i : i + 1, :] * inverse
        x = jnp.where(sub == i, line, jnp.where(sub > i, x - scaled * line, x))
    update = lax.dot_general(
        x[:, :size], x, (((0,), (0,)), ((), ())),
        precision=HIGHEST, preferred_element_type=F32,
    )
    below = iota((size, 2 * size), 0) >= first + PANEL
    work[...] = jnp.where(below, work[...] - update, work[...])
    work[at, :] = x


def cosines(phase, total):
    phase = jnp.where(phase > total // 2, total - phase, phase)
    turned = phase > total // 4
    x = jnp.where(turned, total // 2 - phase, phase).astype(F32) * (2.0 * math.pi / total)
    y = x * x
    value = jnp.full_like(y, 1.0 / math.factorial(12))
    for n in (10, 8, 6, 4, 2, 0):
        value = value * y * (1.0 if n % 4 == 2 else 1.0) + (-1.0) ** (n // 2) / math.factorial(n)
    return jnp.where(turned, -value, value)


def modulo(x, total):
    return x & (total - 1) if total & (total - 1) == 0 else lax.rem(x, total)


def step_kernel(
    n_ma, n_vert, live,
    trial_ref, legendre_ref, order_in, start_in, count_in, weight_in,
    rows_ref, ab_ref, mixer_ref, leg_ref,
    native, leg_in, mine, theirs, far, message, gathered, spectra, returned, packed,
    row_a, land_a, sum_a, row_b, land_b, ab_own, land_c, ab_mid, land_d,
    work, lhs, llm, tables, back_table,
    order_ref, start_ref, count_ref, weight_ref,
    load_sem, leg_sem, small_sem, near_send, near_recv, far_send, far_recv,
    ma_send, ma_recv, vert_send, vert_recv,
):
    ma = lax.axis_index("ma")
    vert = lax.axis_index("vert")
    _, vectors, share, per, _ = native.shape
    orders = n_vert * share
    parts, degrees = mine.shape[2], mine.shape[4]
    tiles = degrees // LANES
    cycles = leg_in.shape[2]
    half = n_vert // 2
    place = lax.rem(vert, half)
    side = vert // half
    assert half == 2
    total = n_vert * vectors
    terms = live * orders
    longitudes = 2 * n_ma * orders

    barrier = pltpu.get_barrier_semaphore()

    def ma_peer(step):
        return lax.rem(ma + step, n_ma)

    def vert_peer(step):
        return lax.rem(vert + step, n_vert)

    def greet_ma(step, carry):
        pl.semaphore_signal(barrier, inc=1, device_id=(ma_peer(step), vert), device_id_type=MESH)
        return carry

    def greet_vert(step, carry):
        pl.semaphore_signal(barrier, inc=1, device_id=(ma, vert_peer(step)), device_id_type=MESH)
        return carry

    lax.fori_loop(1, n_ma, greet_ma, 0)
    lax.fori_loop(1, n_vert, greet_vert, 0)

    def pair_at(i, place=place):
        group = 1 - side if i < half else side
        return group * half + lax.rem(place + i, half)

    def load(i):
        at = pl.ds(pair_at(i) * share, share)
        return pltpu.make_async_copy(trial_ref.at[:, at], native.at[i], load_sem.at[i])

    leg_copy = pltpu.make_async_copy(legendre_ref, leg_in, leg_sem)
    small = [(order_in, order_ref), (start_in, start_ref), (count_in, count_ref), (weight_in, weight_ref)]
    small = [pltpu.make_async_copy(*pair, small_sem.at[n]) for n, pair in enumerate(small)]
    for copy in small:
        copy.start()
    for i in range(n_vert):
        load(i).start()
        if i == half - 1:
            leg_copy.start()

    rows = 8 * per
    row = iota((rows, rows), 0)
    column = iota((rows, rows), 1)
    wanted = modulo(row, 8) * per + modulo(row // 8, tiles) * parts + row // (8 * tiles)
    reorder = (column == wanted).astype(BF16)

    def arrange(i):
        load(i).wait()
        for g in range(vectors // 16):
            for e in range(0, share, 2):
                blocks = []
                for h in range(2):
                    at = pl.ds(16 * g + 8 * h, 8)
                    both = [native[i, at, e + n].reshape(rows, LANES) for n in range(2)]
                    blocks.append(mm(reorder, jnp.concatenate(both, axis=1)))
                for n in range(2):
                    for c in range(parts):
                        for t in range(tiles):
                            lo = (c * tiles + t) * 8
                            at = (slice(lo, lo + 8), slice(n * LANES, (n + 1) * LANES))
                            tile = jnp.concatenate([blocks[0][at], blocks[1][at]], axis=0)
                            at = (slice(16 * g, 16 * g + 16), slice(t * LANES, (t + 1) * LANES))
                            mine[(i, e + n, c) + at] = tile.astype(BF16)

    def near_copy(i, source):
        return pltpu.make_async_remote_copy(
            src_ref=mine.at[i],
            dst_ref=theirs.at[pair_at(i, source)],
            send_sem=near_send.at[i],
            recv_sem=near_recv.at[i],
            device_id=(ma, side * half + 1 - place),
            device_id_type=MESH,
        )

    each = share * parts
    pieces = half * each

    def far_copy(piece, arriving=False):
        offset = piece // each
        inner = lax.rem(piece, each)
        peer = (1 - side) * half + lax.rem(place + offset, half)
        slot = lax.rem(place + half - offset, half) if arriving else place
        s = inner // parts
        c = lax.rem(inner, parts)
        return pltpu.make_async_remote_copy(
            src_ref=mine.at[offset, s, c],
            dst_ref=far.at[slot, s, c],
            send_sem=far_send.at[piece],
            recv_sem=far_recv.at[piece],
            device_id=(ma, peer),
            device_id_type=MESH,
        )

    def send_far(begin, end):
        def body(piece, carry):
            far_copy(piece).start()
            return carry

        lax.fori_loop(begin, end, body, 0)

    cuts = [min(pieces, cut) for cut in STAGES]
    arrange(0)
    pl.semaphore_wait(barrier, n_ma + n_vert - 2)
    send_far(0, min(each, cuts[0]))
    for i in range(1, half):
        arrange(i)
    if cuts[0] > each:
        send_far(each, cuts[0])

    for copy in small:
        copy.wait()

    def search(i, found):
        j = cycles - 1 - i
        return jnp.where(count_ref[j] > 0, j, found)

    first = jnp.minimum(lax.fori_loop(0, cycles, search, 0), cycles - live)

    leg_copy.wait()
    block = min(terms, 64)
    for kind in range(2):
        source = leg_in[:, kind].reshape(orders * cycles, degrees)

        def pick(i, carry):
            row = iota((block, orders * cycles), 0) + i * block
            column = iota((block, orders * cycles), 1)
            wanted = modulo(row, orders) * cycles + row // orders + first
            at = rows_at(kind * (terms // block) + i, block)
            leg_ref[at, :] = mm((column == wanted).astype(BF16), source).astype(BF16)
            return carry

        lax.fori_loop(0, terms // block, pick, 0)

    for i in range(half, n_vert):
        arrange(i)
    for i in range(n_vert):
        near_copy(i, place).start()

    keep = lax.rem(iota((2 * terms, LANES), 0), orders)

    for i in range(n_vert):
        for e in range(share):
            found = mm_nt(leg_ref[...], mine[i, e].reshape(parts * vectors, degrees))
            here = keep == pair_at(i) * share + e
            spectra[...] = jnp.where(here, found, spectra[...]) if i + e else found
    w = spectra[:terms, :]
    x = spectra[terms:, :]
    quarter = iota((terms, LANES), 1) // vectors
    left = lambda a: pltpu.roll(a, LANES - vectors, 1)
    right = lambda a: pltpu.roll(a, vectors, 1)
    w = jnp.where(quarter == 1, left(w), jnp.where(quarter == 2, right(w), w))
    x = jnp.where(quarter == 0, right(x), jnp.where(quarter == 3, left(x), x))
    w = jnp.where((quarter == 1) | (quarter == 3), -w, w)
    fields = w + jnp.where(quarter >= 2, -x, x)
    front = iota((orders, LANES), 1) < LANES // 2
    for pair in range(live // 2):
        a = fields[2 * pair * orders : (2 * pair + 1) * orders]
        b = fields[(2 * pair + 1) * orders : (2 * pair + 2) * orders]
        both = jnp.concatenate([jnp.where(front, a, swap(b)), jnp.where(front, swap(a), b)], axis=0)
        message[:, pair * LANES : (pair + 1) * LANES] = both.astype(BF16)

    def ma_copy(kind, source, target, slot, peer):
        return pltpu.make_async_remote_copy(
            src_ref=source,
            dst_ref=target.at[slot],
            send_sem=ma_send.at[kind, peer],
            recv_sem=ma_recv.at[kind, slot],
            device_id=(peer, vert),
            device_id_type=MESH,
        )

    def over_ma(act):
        def body(step, carry):
            act(ma_peer(step))
            return carry

        lax.fori_loop(1, n_ma, body, 0)

    def ma_start(kind, source, target):
        over_ma(lambda peer: ma_copy(kind, source, target, ma, peer).start())

    def ma_wait(kind, source, target):
        over_ma(lambda peer: ma_copy(kind, source, target, peer, peer).wait_recv())

    def ma_done(kind, source, target):
        over_ma(lambda peer: ma_copy(kind, source, target, ma, peer).wait_send())

    def vert_copy(kind, source, target, slot, peer):
        return pltpu.make_async_remote_copy(
            src_ref=source,
            dst_ref=target.at[slot],
            send_sem=vert_send.at[kind, peer],
            recv_sem=vert_recv.at[kind, slot],
            device_id=(ma, peer),
            device_id_type=MESH,
        )

    def over_vert(act):
        def body(step, carry):
            act(vert_peer(step))
            return carry

        lax.fori_loop(1, n_vert, body, 0)

    def vert_start(kind, source, target):
        over_vert(lambda peer: vert_copy(kind, source, target, vert, peer).start())

    def vert_wait(kind, source, target):
        over_vert(lambda peer: vert_copy(kind, source, target, peer, peer).wait_recv())

    def vert_done(kind, source, target):
        over_vert(lambda peer: vert_copy(kind, source, target, vert, peer).wait_send())

    ma_start(0, message, gathered)
    gathered[ma] = message[...]

    turned = spectra[...].T
    part = [turned[c * vectors : (c + 1) * vectors] for c in range(parts)]
    wide = part[0].shape
    sign = half_sign(wide, 1.0, -1.0)
    field_x = (part[0] + swap(part[3])) * sign
    field_y = part[1] - swap(part[2])
    for n, (piece_x, piece_y) in enumerate(zip(split(field_x, 3), split(field_y, 3))):
        at = slice((3 + n) * vectors, (4 + n) * vectors)
        lhs[at, : 2 * terms] = piece_x
        lhs[at, 2 * terms :] = piece_y

    step_rows = min(2 * terms, LANES)

    def leg_products(i, carry):
        at = rows_at(i, step_rows)
        found = mm_nt(leg_ref[at, :], leg_ref[...])
        same = lax.rem(iota(found.shape, 0) - iota(found.shape, 1) + 2 * terms * orders, orders) == 0
        for n, piece in enumerate(split(jnp.where(same, found, 0.0), 3)):
            llm[n, at, :] = piece
        return carry

    lax.fori_loop(0, 2 * terms // step_rows, leg_products, 0)

    scale = 1.0 / math.sqrt(n_ma * orders)
    width = n_ma * 2 * orders
    lane = iota((8, width), 1)
    slot = lane // (2 * orders) * orders + lax.rem(lane, orders)

    def place_order(i, carry):
        return jnp.where(slot == i, order_ref[i], carry)

    lane_order = lax.fori_loop(0, n_ma * orders, place_order, jnp.zeros((8, width), I32))
    shift = jnp.where(lax.rem(lane // orders, 2) == 1, longitudes - longitudes // 4, 0)

    def table_rows(i, carry):
        j = iota((LANES, width), 0) + i * LANES
        phase = modulo(j * lane_order[:1] + shift[:1], longitudes)
        tables[rows_at(i, LANES), :] = (cosines(phase, longitudes) * scale).astype(BF16)
        return carry

    lax.fori_loop(0, longitudes // LANES, table_rows, 0)
    row = iota((2 * orders, longitudes), 0)
    own_order = jnp.zeros((2 * orders, longitudes), I32)
    for s in range(orders):
        own_order = jnp.where(lax.rem(row, orders) == s, order_ref[ma * orders + s], own_order)
    phase = iota((2 * orders, longitudes), 1) * own_order
    phase = phase + jnp.where(row >= orders, longitudes - longitudes // 4, 0)
    back_table[...] = (cosines(modulo(phase, longitudes), longitudes) * scale).astype(BF16)

    for i in range(n_vert):
        near_copy(i, 1 - place).wait_recv()
    near_sums = jnp.zeros((vectors, half * vectors), F32)
    for i in range(n_vert):
        for e in range(share):
            for c in range(parts):
                here = mine[i, e, c]
                both = jnp.concatenate([here, theirs[pair_at(i), e, c]], axis=0)
                near_sums = near_sums + mm_nt(here, both)
    first_half, second_half = near_sums[:, :vectors], near_sums[:, vectors:]
    swapped = jnp.concatenate([second_half, first_half], axis=1)
    near_sums = jnp.where(place == 0, near_sums, swapped)
    row_b[:, total:] = jnp.concatenate([near_sums, jnp.zeros_like(near_sums)], axis=1)

    ma_wait(0, message, gathered)
    columns = message.shape[1]
    wide_block = min(columns, 512)
    cycles_here = wide_block // (2 * vectors)

    def transform(block, carry):
        at = rows_at(block, wide_block)
        grid = mm(tables[...], gathered[:, :, at].reshape(n_ma * 2 * orders, wide_block))
        lane_cycle = iota((8, wide_block), 1) // (2 * vectors)
        begin = jnp.zeros((8, wide_block), I32)
        length = jnp.zeros((8, wide_block), I32)
        weight = jnp.zeros((8, wide_block), F32)
        for r in range(cycles_here):
            here = lane_cycle == r
            cycle = first + block * cycles_here + r
            begin = jnp.where(here, start_ref[cycle], begin)
            length = jnp.where(here, count_ref[cycle], length)
            weight = jnp.where(here, weight_ref[cycle], weight)
        away = iota(grid.shape, 0) - begin[:1]
        away = jnp.where(away < 0, away + longitudes, away)
        weighted = (grid * jnp.where(away < length[:1], weight[:1], 0.0)).astype(BF16)
        found = mm(back_table[...], weighted)
        for n in range(wide_block // LANES):
            both = found[:, n * LANES : (n + 1) * LANES]
            c, s = both[:orders], both[orders:]
            pair = [jnp.where(front, c, swap(s)), jnp.where(front, swap(c), s)]
            for e in range(2):
                cycle = block * cycles_here + 2 * n + e
                returned[rows_at(cycle, orders), :] = pair[e]
        return carry

    lax.fori_loop(0, columns // wide_block, transform, 0)
    here = returned[...]
    even = lax.rem(iota(here.shape, 1) // vectors, 2) == 0
    turned = jnp.concatenate([here, jnp.where(even, right(here), left(here))], axis=0).T
    turned = turned.astype(BF16)
    g_x = turned[:vectors]
    back_y = turned[vectors : 2 * vectors]
    g_y = turned[2 * vectors : 3 * vectors]
    back_x = turned[3 * vectors :]
    packed[vert, :, : 2 * terms] = g_x
    packed[vert, :, 2 * terms :] = g_y
    vert_start(0, packed.at[vert], packed)
    send_far(cuts[0], cuts[1])

    signs = sign.astype(BF16)
    adjoint = jnp.concatenate([g_x * signs, g_y, -back_y, -back_x * signs], axis=0)
    products = mm(adjoint, llm[0]) + mm(adjoint, llm[1]) + mm(adjoint, llm[2])
    part = [products[c * vectors : (c + 1) * vectors] for c in range(parts)]
    gram_x = part[0] * sign + swap(part[3] * -sign)
    gram_y = part[1] - swap(part[2])
    for n, (piece_x, piece_y) in enumerate(zip(split(gram_x, 3), split(gram_y, 3))):
        at = slice(n * vectors, (n + 1) * vectors)
        lhs[at, : 2 * terms] = piece_x
        lhs[at, 2 * terms :] = piece_y

    vert_wait(0, packed.at[vert], packed)
    everyone = packed[...].reshape(total, 4 * terms)
    found = mm_nt(lhs[...], everyone)
    found = [found[n * vectors : (n + 1) * vectors] for n in range(6)]
    row_a[...] = found[0] + found[1] + found[2]
    ma_start(1, row_a, land_a)
    land_a[ma] = row_a[...]
    row_b[:, :total] = found[3] + found[4] + found[5]
    land_b[ma] = row_b[...]
    ma_wait(1, row_a, land_a)
    sum_a[vert] = jnp.sum(land_a[...], axis=0)
    vert_start(1, sum_a.at[vert], sum_a)
    send_far(cuts[1], pieces)
    ma_start(2, row_b, land_b)
    vert_wait(1, sum_a.at[vert], sum_a)
    inverse_count = 1.0 / (n_ma * orders * parts * degrees)
    work[:, :total] = sum_a[...].reshape(total, total) * inverse_count
    work[:, total:] = (iota((total, total), 0) == iota((total, total), 1)).astype(F32)

    def panel_step(p, carry):
        factor_panel(work, p)
        return carry

    panels = total // PANEL
    lax.fori_loop(0, panels // 2, panel_step, 0)
    ma_wait(2, row_b, land_b)
    rows_ref[vert] = jnp.sum(land_b[...], axis=0)
    vert_start(2, rows_ref.at[vert], rows_ref)

    def far_wait(piece, carry):
        far_copy(piece, True).wait_recv()
        return carry

    lax.fori_loop(0, pieces, far_wait, 0)

    cross_sums = jnp.zeros((half * vectors, half * vectors), F32)
    for e in range(share):
        for c in range(parts):
            here = jnp.concatenate([mine[half, e, c], theirs[vert, e, c]], axis=0)
            there = far[:, e, c].reshape(half * vectors, degrees)
            cross_sums = cross_sums + mm_nt(here, there)
    swapped = jnp.concatenate([cross_sums[vectors:], cross_sums[:vectors]], axis=0)
    cross_sums = jnp.where(place == 0, cross_sums, swapped)
    cross_sums = jnp.where(side == 0, cross_sums, cross_sums.T)
    size = half * vectors
    ab_own[...] = jnp.concatenate([cross_sums[: size // 2], cross_sums[size // 2 :]], axis=1)
    vert_start(3, ab_own, land_c)
    land_c[vert] = ab_own[...]
    lax.fori_loop(panels // 2, panels, panel_step, 0)
    vert_wait(3, ab_own, land_c)
    ab_mid[...] = jnp.sum(land_c[...], axis=0)
    ma_start(3, ab_mid, land_d)
    land_d[ma] = ab_mid[...]

    mixing = work[rows_at(vert, vectors), total:].astype(BF16)
    spread = (iota((parts * vectors, vectors), 0) // parts == iota((parts * vectors, vectors), 1))
    mixing = mm(spread.astype(BF16), mixing).astype(BF16)
    mixed = mm(mixing, everyone)
    mixed_x, mixed_y = mixed[:, : 2 * terms], mixed[:, 2 * terms :]
    kind = lax.rem(iota(mixed_x.shape, 0), parts)
    sign = half_sign(mixed_x.shape, 1.0, -1.0)
    mixer = jnp.where(
        kind == 0, mixed_x * sign,
        jnp.where(kind == 1, mixed_y, jnp.where(kind == 2, -swap(mixed_y), -swap(mixed_x) * sign)),
    )
    high, low = split(mixer, 2)
    mixer_ref[:, : 2 * terms] = high
    mixer_ref[:, 2 * terms :] = low

    vert_wait(2, rows_ref.at[vert], rows_ref)
    ma_wait(3, ab_mid, land_d)
    ab_ref[...] = jnp.sum(land_d[...], axis=0)

    for i in range(n_vert):
        near_copy(i, place).wait_send()

    def far_done(piece, carry):
        far_copy(piece).wait_send()
        return carry

    lax.fori_loop(0, pieces, far_done, 0)
    ma_done(0, message, gathered)
    vert_done(0, packed.at[vert], packed)
    ma_done(1, row_a, land_a)
    ma_done(2, row_b, land_b)
    vert_done(1, sum_a.at[vert], sum_a)
    vert_done(2, rows_ref.at[vert], rows_ref)
    vert_done(3, ab_own, land_c)
    ma_done(3, ab_mid, land_d)


def step_terms(trial, legendre, order_slot, cycle_start, cycle_count, cycle_weight, n_ma, n_vert):
    vectors, orders, per, _ = trial.shape
    _, kinds, cycles, degrees = legendre.shape
    parts = per * LANES // degrees
    live = cycles // 4
    terms = live * orders
    total = n_vert * vectors
    half = n_vert // 2
    share = orders // n_vert
    longitudes = 2 * n_ma * orders
    pieces = half * share * parts
    columns = live * 2 * vectors
    grant = min(60, 16 + terms // 16) * MIB
    anywhere = pl.BlockSpec(memory_space=pltpu.HBM)
    return pl.pallas_call(
        functools.partial(step_kernel, n_ma, n_vert, live),
        out_shape=(
            jax.ShapeDtypeStruct((n_vert, vectors, total + 2 * half * vectors), F32),
            jax.ShapeDtypeStruct((half * vectors // 2, 2 * half * vectors), F32),
            jax.ShapeDtypeStruct((parts * vectors, 4 * terms), BF16),
            jax.ShapeDtypeStruct((2 * terms, degrees), BF16),
        ),
        in_specs=[anywhere] * 6,
        out_specs=[pl.BlockSpec(memory_space=VMEM)] * 4,
        scratch_shapes=[
            VMEM((n_vert, vectors, share, per, LANES), BF16),
            VMEM(legendre.shape, BF16),
            VMEM((n_vert, share, parts, vectors, degrees), BF16),
            VMEM((n_vert, share, parts, vectors, degrees), BF16),
            VMEM((half, share, parts, vectors, degrees), BF16),
            VMEM((2 * orders, columns), BF16),
            VMEM((n_ma, 2 * orders, columns), BF16),
            VMEM((2 * terms, LANES), F32),
            VMEM((terms, LANES), F32),
            VMEM((n_vert, vectors, 4 * terms), BF16),
            VMEM((vectors, total), F32),
            VMEM((n_ma, vectors, total), F32),
            VMEM((n_vert, vectors, total), F32),
            VMEM((vectors, total + 2 * half * vectors), F32),
            VMEM((n_ma, vectors, total + 2 * half * vectors), F32),
            VMEM((half * vectors // 2, 2 * half * vectors), F32),
            VMEM((n_vert, half * vectors // 2, 2 * half * vectors), F32),
            VMEM((half * vectors // 2, 2 * half * vectors), F32),
            VMEM((n_ma, half * vectors // 2, 2 * half * vectors), F32),
            VMEM((total, 2 * total), F32),
            VMEM((6 * vectors, 4 * terms), BF16),
            VMEM((3, 2 * terms, 2 * terms), BF16),
            VMEM((longitudes, n_ma * 2 * orders), BF16),
            VMEM((2 * orders, longitudes), BF16),
            SMEM(order_slot.shape, I32),
            SMEM(cycle_start.shape, I32),
            SMEM(cycle_count.shape, I32),
            SMEM(cycle_weight.shape, F32),
            DMA((n_vert,)),
            DMA,
            DMA((4,)),
            DMA((n_vert,)),
            DMA((n_vert,)),
            DMA((pieces,)),
            DMA((pieces,)),
            DMA((4, n_ma)),
            DMA((4, n_ma)),
            DMA((4, n_vert)),
            DMA((4, n_vert)),
        ],
        compiler_params=pltpu.CompilerParams(
            collective_id=0, has_side_effects=True, vmem_limit_bytes=grant
        ),
        name="step_terms",
    )(trial, legendre, order_slot, cycle_start, cycle_count, cycle_weight)


def finish_kernel(
    coefficients, rows_ref, ab_ref, mixer_ref, leg_ref, basis_ref, ritz_ref, work, staged, sems
):
    total = ritz_ref.shape[0]
    size = total // 2
    orders, vectors, parts, degrees = staged.shape
    scale = 1.0 / coefficients
    own = rows_ref[...].reshape(total, rows_ref.shape[2])
    ab = ab_ref[...]
    ab = jnp.concatenate([ab[:, :size], ab[:, size:]], axis=0)
    top = jnp.concatenate([own[:size, total : total + size], ab], axis=1)
    bottom = jnp.concatenate([ab.T, own[size:, total : total + size]], axis=1)
    work[:, :total] = jnp.concatenate([top, bottom], axis=0) * scale
    work[:, total:] = (iota((total, total), 0) == iota((total, total), 1)).astype(F32)
    mixer = mixer_ref[...]
    lane_order = lax.rem(iota(mixer.shape, 1), orders)

    def out_copy(s):
        return pltpu.make_async_copy(staged.at[s], basis_ref.at[:, s], sems.at[s])

    def mix(s):
        picked = jnp.where(lane_order == s, mixer, jnp.zeros_like(mixer))
        width = mixer.shape[1] // 2
        mixed = mm(picked[:, :width], leg_ref[...]) + mm(picked[:, width:], leg_ref[...])
        staged[s] = mixed.reshape(vectors, parts, degrees).astype(BF16)
        out_copy(s).start()

    panels = total // PANEL
    assert panels == orders

    def step(p, carry):
        factor_panel(work, p)
        mix(p)
        return carry

    lax.fori_loop(0, panels, step, 0)
    inverse = work[:, total:]
    half = jnp.dot(inverse, own[:, :total] * scale, precision=HIGHEST, preferred_element_type=F32)
    ritz_ref[...] = lax.dot_general(
        half, inverse, NT, precision=HIGHEST, preferred_element_type=F32
    )

    def done(s, carry):
        out_copy(s).wait()
        return carry

    lax.fori_loop(0, orders, done, 0)


def finish(rows, ab, mixer, table, vectors, orders, coefficients):
    total = rows.shape[0] * rows.shape[1]
    degrees = table.shape[1]
    parts = mixer.shape[0] // vectors
    return pl.pallas_call(
        functools.partial(finish_kernel, float(coefficients)),
        out_shape=(
            jax.ShapeDtypeStruct((vectors, orders, parts, degrees), BF16),
            jax.ShapeDtypeStruct((total, total), F32),
        ),
        in_specs=[pl.BlockSpec(memory_space=VMEM)] * 4,
        out_specs=(pl.BlockSpec(memory_space=pl.ANY), pl.BlockSpec(memory_space=VMEM)),
        scratch_shapes=[
            VMEM((total, 2 * total), F32),
            VMEM((orders, vectors, parts, degrees), BF16),
            DMA((orders,)),
        ],
        compiler_params=pltpu.CompilerParams(vmem_limit_bytes=32 * 1024 * 1024),
        name="finish",
    )(rows, ab, mixer, table)


def shards(trial_block, legendre, order_slot, cycle_start, cycle_count, cycle_weight):
    n_ma = lax.axis_size("ma")
    n_vert = lax.axis_size("vert")
    vectors, orders, parts, degrees = trial_block.shape
    trial = trial_block.reshape(vectors, orders, parts, degrees // LANES, LANES)
    trial = trial.transpose(0, 1, 3, 2, 4).reshape(vectors, orders, parts * degrees // LANES, LANES)
    inputs = (trial, legendre, order_slot, cycle_start, cycle_count, cycle_weight)
    inputs = [pltpu.with_memory_space_constraint(x, pltpu.HBM) for x in inputs]
    terms = step_terms(*inputs, n_ma, n_vert)
    coefficients = order_slot.shape[0] * parts * degrees
    return finish(*terms, vectors, orders, coefficients)


def solution(mesh):
    in_specs = (P("vert", "ma", None, None), P("ma", None, None, None), P(), P(), P(), P())
    out_specs = (P("vert", "ma", None, None), P())
    return jax.shard_map(shards, mesh=mesh, in_specs=in_specs, out_specs=out_specs, check_vma=False)
```

```python
import functools
import math

import jax
import jax.numpy as jnp
from jax import lax
from jax.experimental import pallas as pl
from jax.experimental.pallas import tpu as pltpu
from jax.sharding import PartitionSpec as P

MESH = pl.DeviceIdType.MESH
VMEM = pltpu.VMEM
SMEM = pltpu.SMEM
DMA = pltpu.SemaphoreType.DMA
F32 = jnp.float32
BF16 = jnp.bfloat16
I32 = jnp.int32
HIGHEST = lax.Precision.HIGHEST
MIB = 1024 * 1024
LANES = 128
PANEL = 16
NT = (((1,), (1,)), ((), ()))
STAGES = (6, 12, 16)


def iota(shape, axis):
    return lax.broadcasted_iota(I32, shape, axis)


def mm(a, b):
    return jnp.dot(a, b, preferred_element_type=F32)


def mm_nt(a, b):
    return lax.dot_general(a, b, NT, preferred_element_type=F32)


def split(x, count):
    pieces = []
    for _ in range(count):
        piece = x.astype(BF16)
        pieces.append(piece)
        x = x - piece.astype(F32)
    return pieces


def swap(x):
    return pltpu.roll(x, x.shape[1] // 2, 1)


def half_sign(shape, first, second):
    return jnp.where(iota(shape, 1) < shape[1] // 2, first, second).astype(F32)


def rows_at(index, count):
    return pl.ds(pl.multiple_of(index * count, count), count)


def factor_panel(work, p):
    size, width = work.shape
    first = pl.multiple_of(p * PANEL, PANEL)
    at = pl.ds(first, PANEL)
    lane = iota((PANEL, size), 1)
    sub = iota((PANEL, width), 0)
    x = work[at, :]
    column = [
        jnp.sum(jnp.where(lane == first + i, x[:, :size], 0.0), axis=1, keepdims=True)
        for i in range(PANEL)
    ]
    for i in range(PANEL):
        inverse = lax.rsqrt(column[i][i : i + 1, :])
        scaled = column[i] * inverse
        for k in range(i + 1, PANEL):
            column[k] = column[k] - scaled * (column[k][i : i + 1, :] * inverse)
        line = x[i : i + 1, :] * inverse
        x = jnp.where(sub == i, line, jnp.where(sub > i, x - scaled * line, x))
    update = lax.dot_general(
        x[:, :size], x, (((0,), (0,)), ((), ())),
        precision=HIGHEST, preferred_element_type=F32,
    )
    below = iota((size, width), 0) >= first + PANEL
    work[...] = jnp.where(below, work[...] - update, work[...])
    work[at, :] = x


def cosines(phase, total):
    phase = jnp.where(phase > total // 2, total - phase, phase)
    turned = phase > total // 4
    x = jnp.where(turned, total // 2 - phase, phase).astype(F32) * (2.0 * math.pi / total)
    y = x * x
    value = jnp.full_like(y, 1.0 / math.factorial(12))
    for n in (10, 8, 6, 4, 2, 0):
        value = value * y * (1.0 if n % 4 == 2 else 1.0) + (-1.0) ** (n // 2) / math.factorial(n)
    return jnp.where(turned, -value, value)


def modulo(x, total):
    return x & (total - 1) if total & (total - 1) == 0 else lax.rem(x, total)


def step_kernel(
    n_ma, n_vert, live,
    trial_ref, legendre_ref, order_in, start_in, count_in, weight_in,
    cross_ref, corner_ref, ab_ref, basis_ref,
    leg_ref, native, leg_in, mine, theirs, far, message, gathered, spectra, returned, packed,
    row_a, land_a, sum_a, row_b, land_b, sum_b, row_e, land_e, sum_e, ab_own, land_c, ab_mid, land_d,
    work, corner, lhs, llm, tables, back_table,
    order_ref, start_ref, count_ref, weight_ref,
    load_sem, leg_sem, small_sem, near_send, near_recv, far_send, far_recv,
    ma_send, ma_recv, vert_send, vert_recv,
):
    ma = lax.axis_index("ma")
    vert = lax.axis_index("vert")
    _, vectors, share, per, _ = native.shape
    orders = n_vert * share
    parts, degrees = mine.shape[2], mine.shape[4]
    tiles = degrees // LANES
    cycles = leg_in.shape[2]
    half = n_vert // 2
    place = lax.rem(vert, half)
    side = vert // half
    assert half == 2
    total = n_vert * vectors
    terms = live * orders
    longitudes = 2 * n_ma * orders

    barrier = pltpu.get_barrier_semaphore()

    def ma_peer(step):
        return lax.rem(ma + step, n_ma)

    def vert_peer(step):
        return lax.rem(vert + step, n_vert)

    def greet_ma(step, carry):
        pl.semaphore_signal(barrier, inc=1, device_id=(ma_peer(step), vert), device_id_type=MESH)
        return carry

    def greet_vert(step, carry):
        pl.semaphore_signal(barrier, inc=1, device_id=(ma, vert_peer(step)), device_id_type=MESH)
        return carry

    lax.fori_loop(1, n_ma, greet_ma, 0)
    lax.fori_loop(1, n_vert, greet_vert, 0)

    def pair_at(i, place=place):
        group = 1 - side if i < half else side
        return group * half + lax.rem(place + i, half)

    def load(i):
        at = pl.ds(pair_at(i) * share, share)
        return pltpu.make_async_copy(trial_ref.at[:, at], native.at[i], load_sem.at[i])

    leg_copy = pltpu.make_async_copy(legendre_ref, leg_in, leg_sem)
    small = [(order_in, order_ref), (start_in, start_ref), (count_in, count_ref), (weight_in, weight_ref)]
    small = [pltpu.make_async_copy(*pair, small_sem.at[n]) for n, pair in enumerate(small)]
    for copy in small:
        copy.start()
    for i in range(n_vert):
        load(i).start()
        if i == half - 1:
            leg_copy.start()

    rows = 8 * per
    row = iota((rows, rows), 0)
    column = iota((rows, rows), 1)
    wanted = modulo(row, 8) * per + modulo(row // 8, tiles) * parts + row // (8 * tiles)
    reorder = (column == wanted).astype(BF16)

    def arrange(i):
        load(i).wait()
        for g in range(vectors // 16):
            for e in range(0, share, 2):
                blocks = []
                for h in range(2):
                    at = pl.ds(16 * g + 8 * h, 8)
                    both = [native[i, at, e + n].reshape(rows, LANES) for n in range(2)]
                    blocks.append(mm(reorder, jnp.concatenate(both, axis=1)))
                for n in range(2):
                    for c in range(parts):
                        for t in range(tiles):
                            lo = (c * tiles + t) * 8
                            at = (slice(lo, lo + 8), slice(n * LANES, (n + 1) * LANES))
                            tile = jnp.concatenate([blocks[0][at], blocks[1][at]], axis=0)
                            at = (slice(16 * g, 16 * g + 16), slice(t * LANES, (t + 1) * LANES))
                            mine[(i, e + n, c) + at] = tile.astype(BF16)

    def near_copy(i, source):
        return pltpu.make_async_remote_copy(
            src_ref=mine.at[i],
            dst_ref=theirs.at[pair_at(i, source)],
            send_sem=near_send.at[i],
            recv_sem=near_recv.at[i],
            device_id=(ma, side * half + 1 - place),
            device_id_type=MESH,
        )

    each = share * parts
    pieces = half * each

    def far_copy(piece, arriving=False):
        offset = piece // each
        inner = lax.rem(piece, each)
        peer = (1 - side) * half + lax.rem(place + offset, half)
        slot = lax.rem(place + half - offset, half) if arriving else place
        s = inner // parts
        c = lax.rem(inner, parts)
        return pltpu.make_async_remote_copy(
            src_ref=mine.at[offset, s, c],
            dst_ref=far.at[slot, s, c],
            send_sem=far_send.at[piece],
            recv_sem=far_recv.at[piece],
            device_id=(ma, peer),
            device_id_type=MESH,
        )

    def send_far(begin, end):
        def body(piece, carry):
            far_copy(piece).start()
            return carry

        lax.fori_loop(begin, end, body, 0)

    cuts = [min(pieces, cut) for cut in STAGES]
    arrange(0)
    pl.semaphore_wait(barrier, n_ma + n_vert - 2)
    send_far(0, min(each, cuts[0]))
    for i in range(1, half):
        arrange(i)
    if cuts[0] > each:
        send_far(each, cuts[0])

    for copy in small:
        copy.wait()

    def search(i, found):
        j = cycles - 1 - i
        return jnp.where(count_ref[j] > 0, j, found)

    first = jnp.minimum(lax.fori_loop(0, cycles, search, 0), cycles - live)

    leg_copy.wait()
    block = min(terms, 64)
    for kind in range(2):
        source = leg_in[:, kind].reshape(orders * cycles, degrees)

        def pick(i, carry):
            row = iota((block, orders * cycles), 0) + i * block
            column = iota((block, orders * cycles), 1)
            wanted = modulo(row, orders) * cycles + row // orders + first
            at = rows_at(kind * (terms // block) + i, block)
            leg_ref[at, :] = mm((column == wanted).astype(BF16), source).astype(BF16)
            return carry

        lax.fori_loop(0, terms // block, pick, 0)

    for i in range(half, n_vert):
        arrange(i)
    for i in range(n_vert):
        near_copy(i, place).start()

    keep = lax.rem(iota((2 * terms, LANES), 0), orders)

    for i in range(n_vert):
        both = mm_nt(leg_ref[...], mine[i].reshape(share * parts * vectors, degrees))
        for e in range(share):
            found = both[:, e * LANES : (e + 1) * LANES]
            here = keep == pair_at(i) * share + e
            spectra[...] = jnp.where(here, found, spectra[...]) if i + e else found
    w = spectra[:terms, :]
    x = spectra[terms:, :]
    quarter = iota((terms, LANES), 1) // vectors
    left = lambda a: pltpu.roll(a, LANES - vectors, 1)
    right = lambda a: pltpu.roll(a, vectors, 1)
    w = jnp.where(quarter == 1, left(w), jnp.where(quarter == 2, right(w), w))
    x = jnp.where(quarter == 0, right(x), jnp.where(quarter == 3, left(x), x))
    w = jnp.where((quarter == 1) | (quarter == 3), -w, w)
    fields = w + jnp.where(quarter >= 2, -x, x)
    front = iota((orders, LANES), 1) < LANES // 2
    for pair in range(live // 2):
        a = fields[2 * pair * orders : (2 * pair + 1) * orders]
        b = fields[(2 * pair + 1) * orders : (2 * pair + 2) * orders]
        both = jnp.concatenate([jnp.where(front, a, swap(b)), jnp.where(front, swap(a), b)], axis=0)
        message[:, pair * LANES : (pair + 1) * LANES] = both.astype(BF16)

    def ma_copy(kind, source, target, slot, peer):
        return pltpu.make_async_remote_copy(
            src_ref=source,
            dst_ref=target.at[slot],
            send_sem=ma_send.at[kind, peer],
            recv_sem=ma_recv.at[kind, slot],
            device_id=(peer, vert),
            device_id_type=MESH,
        )

    def over_ma(act):
        def body(step, carry):
            act(ma_peer(step))
            return carry

        lax.fori_loop(1, n_ma, body, 0)

    def ma_start(kind, source, target):
        over_ma(lambda peer: ma_copy(kind, source, target, ma, peer).start())

    def ma_wait(kind, source, target):
        over_ma(lambda peer: ma_copy(kind, source, target, peer, peer).wait_recv())

    def ma_done(kind, source, target):
        over_ma(lambda peer: ma_copy(kind, source, target, ma, peer).wait_send())

    def vert_copy(kind, source, target, slot, peer):
        return pltpu.make_async_remote_copy(
            src_ref=source,
            dst_ref=target.at[slot],
            send_sem=vert_send.at[kind, peer],
            recv_sem=vert_recv.at[kind, slot],
            device_id=(ma, peer),
            device_id_type=MESH,
        )

    def over_vert(act):
        def body(step, carry):
            act(vert_peer(step))
            return carry

        lax.fori_loop(1, n_vert, body, 0)

    def vert_start(kind, source, target):
        over_vert(lambda peer: vert_copy(kind, source, target, vert, peer).start())

    def vert_wait(kind, source, target):
        over_vert(lambda peer: vert_copy(kind, source, target, peer, peer).wait_recv())

    def vert_done(kind, source, target):
        over_vert(lambda peer: vert_copy(kind, source, target, vert, peer).wait_send())

    ma_start(0, message, gathered)
    gathered[ma] = message[...]

    turned = spectra[...].T
    part = [turned[c * vectors : (c + 1) * vectors] for c in range(parts)]
    wide = part[0].shape
    sign = half_sign(wide, 1.0, -1.0)
    field_x = (part[0] + swap(part[3])) * sign
    field_y = part[1] - swap(part[2])
    for n, (piece_x, piece_y) in enumerate(zip(split(field_x, 3), split(field_y, 3))):
        at = slice((3 + n) * vectors, (4 + n) * vectors)
        lhs[at, : 2 * terms] = piece_x
        lhs[at, 2 * terms :] = piece_y

    step_rows = min(2 * terms, LANES)

    def leg_products(i, carry):
        at = rows_at(i, step_rows)
        found = mm_nt(leg_ref[at, :], leg_ref[...])
        same = lax.rem(iota(found.shape, 0) - iota(found.shape, 1) + 2 * terms * orders, orders) == 0
        for n, piece in enumerate(split(jnp.where(same, found, 0.0), 3)):
            llm[n, at, :] = piece
        return carry

    lax.fori_loop(0, 2 * terms // step_rows, leg_products, 0)

    scale = 1.0 / math.sqrt(n_ma * orders)
    width = n_ma * 2 * orders
    lane = iota((8, width), 1)
    slot = lane // (2 * orders) * orders + lax.rem(lane, orders)

    def place_order(i, carry):
        return jnp.where(slot == i, order_ref[i], carry)

    lane_order = lax.fori_loop(0, n_ma * orders, place_order, jnp.zeros((8, width), I32))
    shift = jnp.where(lax.rem(lane // orders, 2) == 1, longitudes - longitudes // 4, 0)

    def table_rows(i, carry):
        j = iota((LANES, width), 0) + i * LANES
        phase = modulo(j * lane_order[:1] + shift[:1], longitudes)
        tables[rows_at(i, LANES), :] = (cosines(phase, longitudes) * scale).astype(BF16)
        return carry

    lax.fori_loop(0, longitudes // LANES, table_rows, 0)
    row = iota((2 * orders, longitudes), 0)
    own_order = jnp.zeros((2 * orders, longitudes), I32)
    for s in range(orders):
        own_order = jnp.where(lax.rem(row, orders) == s, order_ref[ma * orders + s], own_order)
    phase = iota((2 * orders, longitudes), 1) * own_order
    phase = phase + jnp.where(row >= orders, longitudes - longitudes // 4, 0)
    back_table[...] = (cosines(modulo(phase, longitudes), longitudes) * scale).astype(BF16)

    ma_wait(0, message, gathered)
    columns = message.shape[1]
    wide_block = min(columns, 512)
    cycles_here = wide_block // (2 * vectors)

    def transform(block, carry):
        at = rows_at(block, wide_block)
        grid = mm(tables[...], gathered[:, :, at].reshape(n_ma * 2 * orders, wide_block))
        lane_cycle = iota((8, wide_block), 1) // (2 * vectors)
        begin = jnp.zeros((8, wide_block), I32)
        length = jnp.zeros((8, wide_block), I32)
        weight = jnp.zeros((8, wide_block), F32)
        for r in range(cycles_here):
            here = lane_cycle == r
            cycle = first + block * cycles_here + r
            begin = jnp.where(here, start_ref[cycle], begin)
            length = jnp.where(here, count_ref[cycle], length)
            weight = jnp.where(here, weight_ref[cycle], weight)
        away = iota(grid.shape, 0) - begin[:1]
        away = jnp.where(away < 0, away + longitudes, away)
        weighted = (grid * jnp.where(away < length[:1], weight[:1], 0.0)).astype(BF16)
        found = mm(back_table[...], weighted)
        for n in range(wide_block // LANES):
            both = found[:, n * LANES : (n + 1) * LANES]
            c, s = both[:orders], both[orders:]
            pair = [jnp.where(front, c, swap(s)), jnp.where(front, swap(c), s)]
            for e in range(2):
                cycle = block * cycles_here + 2 * n + e
                returned[rows_at(cycle, orders), :] = pair[e]
        return carry

    lax.fori_loop(0, columns // wide_block, transform, 0)
    here = returned[...]
    even = lax.rem(iota(here.shape, 1) // vectors, 2) == 0
    turned = jnp.concatenate([here, jnp.where(even, right(here), left(here))], axis=0).T
    turned = turned.astype(BF16)
    g_x = turned[:vectors]
    back_y = turned[vectors : 2 * vectors]
    g_y = turned[2 * vectors : 3 * vectors]
    back_x = turned[3 * vectors :]
    packed[vert, :, : 2 * terms] = g_x
    packed[vert, :, 2 * terms :] = g_y
    vert_start(0, packed.at[vert], packed)
    send_far(cuts[0], cuts[1])

    signs = sign.astype(BF16)
    adjoint = jnp.concatenate([g_x * signs, g_y, -back_y, -back_x * signs], axis=0)
    products = mm(adjoint, llm[0]) + mm(adjoint, llm[1]) + mm(adjoint, llm[2])
    part = [products[c * vectors : (c + 1) * vectors] for c in range(parts)]
    gram_x = part[0] * sign + swap(part[3] * -sign)
    gram_y = part[1] - swap(part[2])
    for n, (piece_x, piece_y) in enumerate(zip(split(gram_x, 3), split(gram_y, 3))):
        at = slice(n * vectors, (n + 1) * vectors)
        lhs[at, : 2 * terms] = piece_x
        lhs[at, 2 * terms :] = piece_y

    vert_wait(0, packed.at[vert], packed)
    everyone = packed[...].reshape(total, 4 * terms)
    found = mm_nt(lhs[...], everyone)
    found = [found[n * vectors : (n + 1) * vectors] for n in range(6)]
    row_a[...] = found[0] + found[1] + found[2]
    ma_start(1, row_a, land_a)
    land_a[ma] = row_a[...]
    row_b[...] = found[3] + found[4] + found[5]
    land_b[ma] = row_b[...]

    for i in range(n_vert):
        near_copy(i, 1 - place).wait_recv()
    wide = parts * vectors
    near_sums = jnp.zeros((wide, 2 * wide), F32)
    for i in range(n_vert):
        for e in range(share):
            here = mine[i, e].reshape(wide, degrees)
            both = jnp.concatenate([here, theirs[pair_at(i), e].reshape(wide, degrees)], axis=0)
            near_sums = near_sums + mm_nt(here, both)
    first_half, second_half = [
        sum(
            near_sums[c * vectors : (c + 1) * vectors, n * wide + c * vectors : n * wide + (c + 1) * vectors]
            for c in range(parts)
        )
        for n in range(2)
    ]
    near_sums = jnp.concatenate([first_half, second_half], axis=1)
    swapped = jnp.concatenate([second_half, first_half], axis=1)
    near_sums = jnp.where(place == 0, near_sums, swapped)
    row_e[...] = jnp.concatenate([near_sums[: vectors // 2], near_sums[vectors // 2 :]], axis=1)
    ma_start(4, row_e, land_e)
    land_e[ma] = row_e[...]

    ma_wait(1, row_a, land_a)
    sum_a[vert] = jnp.sum(land_a[...], axis=0)
    vert_start(1, sum_a.at[vert], sum_a)
    send_far(cuts[1], cuts[2])
    ma_start(2, row_b, land_b)
    ma_wait(4, row_e, land_e)
    sum_e[vert] = jnp.sum(land_e[...], axis=0)
    vert_start(4, sum_e.at[vert], sum_e)
    send_far(cuts[2], pieces)

    vert_wait(1, sum_a.at[vert], sum_a)
    inverse_count = 1.0 / (n_ma * orders * parts * degrees)
    work[:, :total] = sum_a[...].reshape(total, total) * inverse_count
    work[:, total:] = (iota((total, total), 0) == iota((total, total), 1)).astype(F32)

    def panel_step(p, carry):
        factor_panel(work, p)
        return carry

    panels = total // PANEL
    lax.fori_loop(0, panels, panel_step, 0)

    ma_wait(2, row_b, land_b)
    sum_b[vert] = jnp.sum(land_b[...], axis=0)

    def far_wait(piece, carry):
        far_copy(piece, True).wait_recv()
        return carry

    lax.fori_loop(0, pieces, far_wait, 0)

    cross_sums = jnp.zeros((2 * wide, 2 * wide), F32)
    for e in range(share):
        here = [mine[half, e].reshape(wide, degrees), theirs[vert, e].reshape(wide, degrees)]
        there = far[:, e].reshape(half * wide, degrees)
        cross_sums = cross_sums + mm_nt(jnp.concatenate(here, axis=0), there)
    cross_sums = jnp.concatenate(
        [
            jnp.concatenate(
                [
                    sum(
                        cross_sums[
                            m * wide + c * vectors : m * wide + (c + 1) * vectors,
                            n * wide + c * vectors : n * wide + (c + 1) * vectors,
                        ]
                        for c in range(parts)
                    )
                    for n in range(2)
                ],
                axis=1,
            )
            for m in range(2)
        ],
        axis=0,
    )
    swapped = jnp.concatenate([cross_sums[vectors:], cross_sums[:vectors]], axis=0)
    cross_sums = jnp.where(place == 0, cross_sums, swapped)
    cross_sums = jnp.where(side == 0, cross_sums, cross_sums.T)
    size = half * vectors
    ab_own[...] = jnp.concatenate([cross_sums[: size // 2], cross_sums[size // 2 :]], axis=1)
    vert_start(3, ab_own, land_c)
    land_c[vert] = ab_own[...]

    vert_wait(4, sum_e.at[vert], sum_e)
    blocks = sum_e[...]
    size = half * vectors
    near_blocks = [
        jnp.concatenate([blocks[n][:, :size], blocks[n][:, size:]], axis=0) * inverse_count
        for n in range(n_vert)
    ]
    diagonals = [jnp.concatenate(near_blocks[n * half : (n + 1) * half], axis=0) for n in range(2)]
    unit = (iota((size, size), 0) == iota((size, size), 1)).astype(F32)
    corner[...] = jnp.concatenate([diagonals[0], unit], axis=1)

    def corner_step(p, carry):
        factor_panel(corner, p)
        return carry

    lax.fori_loop(0, size // PANEL, corner_step, 0)
    in_front = iota(corner.shape, 1) < size
    inverse = jnp.where(in_front, swap(corner[...]), 0.0)
    corner_ref[...] = jnp.concatenate([inverse[:, :size], diagonals[1]], axis=1)

    vert_wait(3, ab_own, land_c)
    ab_mid[...] = jnp.sum(land_c[...], axis=0)
    ma_start(3, ab_mid, land_d)
    land_d[ma] = ab_mid[...]
    vert_start(2, sum_b.at[vert], sum_b)

    mixing = work[rows_at(vert, vectors), total:].astype(BF16)
    spread = (iota((parts * vectors, vectors), 0) // parts == iota((parts * vectors, vectors), 1))
    mixing = mm(spread.astype(BF16), mixing).astype(BF16)
    mixed = mm(mixing, everyone)
    mixed_x, mixed_y = mixed[:, : 2 * terms], mixed[:, 2 * terms :]
    kind = lax.rem(iota(mixed_x.shape, 0), parts)
    sign = half_sign(mixed_x.shape, 1.0, -1.0)
    mixer = jnp.where(
        kind == 0, mixed_x * sign,
        jnp.where(kind == 1, mixed_y, jnp.where(kind == 2, -swap(mixed_y), -swap(mixed_x) * sign)),
    )
    pieces_of = split(mixer, 2)
    lane_order = modulo(iota(mixer.shape, 1), orders)

    def mix(s, carry):
        chosen = [jnp.where(lane_order == s, piece, jnp.zeros_like(piece)) for piece in pieces_of]
        mixed = mm(chosen[0], leg_ref[...]) + mm(chosen[1], leg_ref[...])
        basis_ref[:, s] = mixed.reshape(vectors, parts, degrees).astype(BF16)
        return carry

    lax.fori_loop(0, orders, mix, 0)

    vert_wait(2, sum_b.at[vert], sum_b)
    lower = (iota((size, total), 0) + size == iota((size, total), 1)).astype(F32)
    outer = jnp.concatenate([inverse, lower], axis=0)
    crossed = jnp.dot(
        outer, sum_b[...].reshape(total, total) * inverse_count,
        precision=HIGHEST, preferred_element_type=F32,
    )
    cross_ref[...] = lax.dot_general(
        crossed, outer, NT, precision=HIGHEST, preferred_element_type=F32
    )
    ma_wait(3, ab_mid, land_d)
    ab_ref[...] = jnp.sum(land_d[...], axis=0) * inverse_count

    for i in range(n_vert):
        near_copy(i, place).wait_send()

    def far_done(piece, carry):
        far_copy(piece).wait_send()
        return carry

    lax.fori_loop(0, pieces, far_done, 0)
    ma_done(0, message, gathered)
    vert_done(0, packed.at[vert], packed)
    ma_done(1, row_a, land_a)
    ma_done(2, row_b, land_b)
    vert_done(1, sum_a.at[vert], sum_a)
    vert_done(2, sum_b.at[vert], sum_b)
    ma_done(4, row_e, land_e)
    vert_done(4, sum_e.at[vert], sum_e)
    vert_done(3, ab_own, land_c)
    ma_done(3, ab_mid, land_d)


def step_terms(trial, legendre, order_slot, cycle_start, cycle_count, cycle_weight, n_ma, n_vert):
    vectors, orders, per, _ = trial.shape
    _, kinds, cycles, degrees = legendre.shape
    parts = per * LANES // degrees
    live = cycles // 4
    terms = live * orders
    total = n_vert * vectors
    half = n_vert // 2
    share = orders // n_vert
    longitudes = 2 * n_ma * orders
    pieces = half * share * parts
    columns = live * 2 * vectors
    grant = min(60, 16 + terms // 16) * MIB
    anywhere = pl.BlockSpec(memory_space=pltpu.HBM)
    return pl.pallas_call(
        functools.partial(step_kernel, n_ma, n_vert, live),
        out_shape=(
            jax.ShapeDtypeStruct((total, total), F32),
            jax.ShapeDtypeStruct((half * vectors, 2 * half * vectors), F32),
            jax.ShapeDtypeStruct((half * vectors // 2, 2 * half * vectors), F32),
            jax.ShapeDtypeStruct((vectors, orders, parts, degrees), BF16),
        ),
        in_specs=[anywhere] * 6,
        out_specs=[pl.BlockSpec(memory_space=VMEM)] * 4,
        scratch_shapes=[
            VMEM((2 * terms, degrees), BF16),
            VMEM((n_vert, vectors, share, per, LANES), BF16),
            VMEM(legendre.shape, BF16),
            VMEM((n_vert, share, parts, vectors, degrees), BF16),
            VMEM((n_vert, share, parts, vectors, degrees), BF16),
            VMEM((half, share, parts, vectors, degrees), BF16),
            VMEM((2 * orders, columns), BF16),
            VMEM((n_ma, 2 * orders, columns), BF16),
            VMEM((2 * terms, LANES), F32),
            VMEM((terms, LANES), F32),
            VMEM((n_vert, vectors, 4 * terms), BF16),
            VMEM((vectors, total), F32),
            VMEM((n_ma, vectors, total), F32),
            VMEM((n_vert, vectors, total), F32),
            VMEM((vectors, total), F32),
            VMEM((n_ma, vectors, total), F32),
            VMEM((n_vert, vectors, total), F32),
            VMEM((vectors // 2, 2 * half * vectors), F32),
            VMEM((n_ma, vectors // 2, 2 * half * vectors), F32),
            VMEM((n_vert, vectors // 2, 2 * half * vectors), F32),
            VMEM((half * vectors // 2, 2 * half * vectors), F32),
            VMEM((n_vert, half * vectors // 2, 2 * half * vectors), F32),
            VMEM((half * vectors // 2, 2 * half * vectors), F32),
            VMEM((n_ma, half * vectors // 2, 2 * half * vectors), F32),
            VMEM((total, 2 * total), F32),
            VMEM((half * vectors, 2 * half * vectors), F32),
            VMEM((6 * vectors, 4 * terms), BF16),
            VMEM((3, 2 * terms, 2 * terms), BF16),
            VMEM((longitudes, n_ma * 2 * orders), BF16),
            VMEM((2 * orders, longitudes), BF16),
            SMEM(order_slot.shape, I32),
            SMEM(cycle_start.shape, I32),
            SMEM(cycle_count.shape, I32),
            SMEM(cycle_weight.shape, F32),
            DMA((n_vert,)),
            DMA,
            DMA((4,)),
            DMA((n_vert,)),
            DMA((n_vert,)),
            DMA((pieces,)),
            DMA((pieces,)),
            DMA((5, n_ma)),
            DMA((5, n_ma)),
            DMA((5, n_vert)),
            DMA((5, n_vert)),
        ],
        compiler_params=pltpu.CompilerParams(
            collective_id=0, has_side_effects=True, vmem_limit_bytes=grant
        ),
        name="step_terms",
    )(trial, legendre, order_slot, cycle_start, cycle_count, cycle_weight)


def finish_kernel(cross_ref, corner_ref, ab_ref, staged_ref, basis_ref, ritz_ref, work, sem):
    total = ritz_ref.shape[0]
    size = total // 2
    out = pltpu.make_async_copy(staged_ref, basis_ref, sem)
    out.start()
    ab = ab_ref[...]
    ab = jnp.concatenate([ab[:, :size], ab[:, size:]], axis=0)
    inverse, diagonal = corner_ref[:, :size], corner_ref[:, size:]
    beside = jnp.dot(inverse, ab, precision=HIGHEST, preferred_element_type=F32)
    taken = lax.dot_general(
        beside, beside, (((0,), (0,)), ((), ())), precision=HIGHEST, preferred_element_type=F32
    )
    unit = (iota((size, size), 0) == iota((size, size), 1)).astype(F32)
    work[:, :total] = jnp.concatenate([diagonal - taken, jnp.zeros_like(unit)], axis=1)
    work[:, total:] = jnp.concatenate([-beside.T, unit], axis=1)

    def step(p, carry):
        factor_panel(work, p)
        return carry

    lax.fori_loop(0, size // PANEL, step, 0)
    upper = (iota((size, total), 0) == iota((size, total), 1)).astype(F32)
    outer = jnp.concatenate([upper, work[:, total:]], axis=0)
    crossed = jnp.dot(outer, cross_ref[...], precision=HIGHEST, preferred_element_type=F32)
    ritz_ref[...] = lax.dot_general(
        crossed, outer, NT, precision=HIGHEST, preferred_element_type=F32
    )
    out.wait()


def finish(cross, corner, ab, staged):
    total = cross.shape[0]
    return pl.pallas_call(
        finish_kernel,
        out_shape=(
            jax.ShapeDtypeStruct(staged.shape, BF16),
            jax.ShapeDtypeStruct((total, total), F32),
        ),
        in_specs=[pl.BlockSpec(memory_space=VMEM)] * 4,
        out_specs=(pl.BlockSpec(memory_space=pl.ANY), pl.BlockSpec(memory_space=VMEM)),
        scratch_shapes=[VMEM((total // 2, 2 * total), F32), DMA],
        compiler_params=pltpu.CompilerParams(vmem_limit_bytes=8 * MIB),
        name="finish",
    )(cross, corner, ab, staged)


def shards(trial_block, legendre, order_slot, cycle_start, cycle_count, cycle_weight):
    n_ma = lax.axis_size("ma")
    n_vert = lax.axis_size("vert")
    vectors, orders, parts, degrees = trial_block.shape
    trial = trial_block.reshape(vectors, orders, parts, degrees // LANES, LANES)
    trial = trial.transpose(0, 1, 3, 2, 4).reshape(vectors, orders, parts * degrees // LANES, LANES)
    inputs = (trial, legendre, order_slot, cycle_start, cycle_count, cycle_weight)
    inputs = [pltpu.with_memory_space_constraint(x, pltpu.HBM) for x in inputs]
    return finish(*step_terms(*inputs, n_ma, n_vert))


def solution(mesh):
    in_specs = (P("vert", "ma", None, None), P("ma", None, None, None), P(), P(), P(), P())
    out_specs = (P("vert", "ma", None, None), P())
    return jax.shard_map(shards, mesh=mesh, in_specs=in_specs, out_specs=out_specs, check_vma=False)
```

```python
import functools
import math

import jax
import jax.numpy as jnp
from jax import lax
from jax.experimental import pallas as pl
from jax.experimental.pallas import tpu as pltpu
from jax.sharding import PartitionSpec as P

MESH = pl.DeviceIdType.MESH
VMEM = pltpu.VMEM
SMEM = pltpu.SMEM
DMA = pltpu.SemaphoreType.DMA
F32 = jnp.float32
BF16 = jnp.bfloat16
I32 = jnp.int32
HIGHEST = lax.Precision.HIGHEST
MIB = 1024 * 1024
LANES = 128
PANEL = 16
NT = (((1,), (1,)), ((), ()))
STAGES = (6, 13, 14)


def iota(shape, axis):
    return lax.broadcasted_iota(I32, shape, axis)


def mm(a, b):
    return jnp.dot(a, b, preferred_element_type=F32)


def mm_nt(a, b):
    return lax.dot_general(a, b, NT, preferred_element_type=F32)


def split(x, count):
    pieces = []
    for _ in range(count):
        piece = x.astype(BF16)
        pieces.append(piece)
        x = x - piece.astype(F32)
    return pieces


def swap(x):
    return pltpu.roll(x, x.shape[1] // 2, 1)


def half_sign(shape, first, second):
    return jnp.where(iota(shape, 1) < shape[1] // 2, first, second).astype(F32)


def rows_at(index, count):
    return pl.ds(pl.multiple_of(index * count, count), count)


def factor_panel(work, p):
    size, width = work.shape
    first = pl.multiple_of(p * PANEL, PANEL)
    at = pl.ds(first, PANEL)
    lane = iota((PANEL, size), 1)
    sub = iota((PANEL, width), 0)
    x = work[at, :]
    column = [
        jnp.sum(jnp.where(lane == first + i, x[:, :size], 0.0), axis=1, keepdims=True)
        for i in range(PANEL)
    ]
    for i in range(PANEL):
        inverse = lax.rsqrt(column[i][i : i + 1, :])
        scaled = column[i] * inverse
        for k in range(i + 1, PANEL):
            column[k] = column[k] - scaled * (column[k][i : i + 1, :] * inverse)
        line = x[i : i + 1, :] * inverse
        x = jnp.where(sub == i, line, jnp.where(sub > i, x - scaled * line, x))
    high, middle, low = split(x, 3)
    left = jnp.concatenate([high, high, high, middle, middle, low], axis=0)
    right = jnp.concatenate([high, middle, low, high, middle, high], axis=0)
    update = lax.dot_general(
        left[:, :size], right, (((0,), (0,)), ((), ())), preferred_element_type=F32
    )
    below = iota((size, width), 0) >= first + PANEL
    work[...] = jnp.where(below, work[...] - update, work[...])
    work[at, :] = x


def cosines(phase, total):
    phase = jnp.where(phase > total // 2, total - phase, phase)
    turned = phase > total // 4
    x = jnp.where(turned, total // 2 - phase, phase).astype(F32) * (2.0 * math.pi / total)
    y = x * x
    value = jnp.full_like(y, 1.0 / math.factorial(12))
    for n in (10, 8, 6, 4, 2, 0):
        value = value * y * (1.0 if n % 4 == 2 else 1.0) + (-1.0) ** (n // 2) / math.factorial(n)
    return jnp.where(turned, -value, value)


def modulo(x, total):
    return x & (total - 1) if total & (total - 1) == 0 else lax.rem(x, total)


def step_kernel(
    n_ma, n_vert, live,
    trial_ref, legendre_ref, order_in, start_in, count_in, weight_in,
    cross_ref, corner_ref, ab_ref, basis_ref,
    leg_ref, native, leg_in, mine, theirs, far, message, gathered, spectra, returned, packed,
    row_a, land_a, sum_a, row_b, land_b, sum_b, row_e, land_e, sum_e, ab_own, land_c, ab_mid, land_d,
    work, corner, lhs, llm, tables, back_table,
    order_ref, start_ref, count_ref, weight_ref,
    load_sem, leg_sem, small_sem, near_send, near_recv, far_send, far_recv,
    ma_send, ma_recv, vert_send, vert_recv,
):
    ma = lax.axis_index("ma")
    vert = lax.axis_index("vert")
    _, vectors, share, per, _ = native.shape
    orders = n_vert * share
    parts, degrees = mine.shape[2], mine.shape[4]
    tiles = degrees // LANES
    cycles = leg_in.shape[2]
    half = n_vert // 2
    place = lax.rem(vert, half)
    side = vert // half
    assert half == 2
    total = n_vert * vectors
    terms = live * orders
    longitudes = 2 * n_ma * orders

    barrier = pltpu.get_barrier_semaphore()

    def ma_peer(step):
        return lax.rem(ma + step, n_ma)

    def vert_peer(step):
        return lax.rem(vert + step, n_vert)

    def greet_ma(step, carry):
        pl.semaphore_signal(barrier, inc=1, device_id=(ma_peer(step), vert), device_id_type=MESH)
        return carry

    def greet_vert(step, carry):
        pl.semaphore_signal(barrier, inc=1, device_id=(ma, vert_peer(step)), device_id_type=MESH)
        return carry

    lax.fori_loop(1, n_ma, greet_ma, 0)
    lax.fori_loop(1, n_vert, greet_vert, 0)

    def pair_at(i, place=place):
        group = 1 - side if i < half else side
        return group * half + lax.rem(place + i, half)

    def load(i):
        at = pl.ds(pair_at(i) * share, share)
        return pltpu.make_async_copy(trial_ref.at[:, at], native.at[i], load_sem.at[i])

    leg_copy = pltpu.make_async_copy(legendre_ref, leg_in, leg_sem)
    small = [(order_in, order_ref), (start_in, start_ref), (count_in, count_ref), (weight_in, weight_ref)]
    small = [pltpu.make_async_copy(*pair, small_sem.at[n]) for n, pair in enumerate(small)]
    for copy in small:
        copy.start()
    for i in range(n_vert):
        load(i).start()
        if i == half - 1:
            leg_copy.start()

    rows = 8 * per
    row = iota((rows, rows), 0)
    column = iota((rows, rows), 1)
    wanted = modulo(row, 8) * per + modulo(row // 8, tiles) * parts + row // (8 * tiles)
    reorder = (column == wanted).astype(BF16)

    def arrange(i):
        load(i).wait()
        for g in range(vectors // 16):
            for e in range(0, share, 2):
                blocks = []
                for h in range(2):
                    at = pl.ds(16 * g + 8 * h, 8)
                    both = [native[i, at, e + n].reshape(rows, LANES) for n in range(2)]
                    blocks.append(mm(reorder, jnp.concatenate(both, axis=1)))
                for n in range(2):
                    for c in range(parts):
                        for t in range(tiles):
                            lo = (c * tiles + t) * 8
                            at = (slice(lo, lo + 8), slice(n * LANES, (n + 1) * LANES))
                            tile = jnp.concatenate([blocks[0][at], blocks[1][at]], axis=0)
                            at = (slice(16 * g, 16 * g + 16), slice(t * LANES, (t + 1) * LANES))
                            mine[(i, e + n, c) + at] = tile.astype(BF16)

    def near_copy(i, source):
        return pltpu.make_async_remote_copy(
            src_ref=mine.at[i],
            dst_ref=theirs.at[pair_at(i, source)],
            send_sem=near_send.at[i],
            recv_sem=near_recv.at[i],
            device_id=(ma, side * half + 1 - place),
            device_id_type=MESH,
        )

    each = share * parts
    pieces = half * each

    def far_copy(piece, arriving=False):
        offset = piece // each
        inner = lax.rem(piece, each)
        peer = (1 - side) * half + lax.rem(place + offset, half)
        slot = lax.rem(place + half - offset, half) if arriving else place
        s = inner // parts
        c = lax.rem(inner, parts)
        return pltpu.make_async_remote_copy(
            src_ref=mine.at[offset, s, c],
            dst_ref=far.at[slot, s, c],
            send_sem=far_send.at[piece],
            recv_sem=far_recv.at[piece],
            device_id=(ma, peer),
            device_id_type=MESH,
        )

    def send_far(begin, end):
        def body(piece, carry):
            far_copy(piece).start()
            return carry

        lax.fori_loop(begin, end, body, 0)

    cuts = [min(pieces, cut) for cut in STAGES]
    arrange(0)
    pl.semaphore_wait(barrier, n_ma + n_vert - 2)
    send_far(0, min(each, cuts[0]))
    for i in range(1, half):
        arrange(i)
    if cuts[0] > each:
        send_far(each, cuts[0])

    for copy in small:
        copy.wait()

    def search(i, found):
        j = cycles - 1 - i
        return jnp.where(count_ref[j] > 0, j, found)

    first = jnp.minimum(lax.fori_loop(0, cycles, search, 0), cycles - live)

    leg_copy.wait()
    block = min(terms, 64)
    for kind in range(2):
        source = leg_in[:, kind].reshape(orders * cycles, degrees)

        def pick(i, carry):
            row = iota((block, orders * cycles), 0) + i * block
            column = iota((block, orders * cycles), 1)
            wanted = modulo(row, orders) * cycles + row // orders + first
            at = rows_at(kind * (terms // block) + i, block)
            leg_ref[at, :] = mm((column == wanted).astype(BF16), source).astype(BF16)
            return carry

        lax.fori_loop(0, terms // block, pick, 0)

    for i in range(half, n_vert):
        arrange(i)
    for i in range(n_vert):
        near_copy(i, place).start()

    keep = lax.rem(iota((2 * terms, LANES), 0), orders)

    for i in range(n_vert):
        both = mm_nt(leg_ref[...], mine[i].reshape(share * parts * vectors, degrees))
        for e in range(share):
            found = both[:, e * LANES : (e + 1) * LANES]
            here = keep == pair_at(i) * share + e
            spectra[...] = jnp.where(here, found, spectra[...]) if i + e else found
    w = spectra[:terms, :]
    x = spectra[terms:, :]
    quarter = iota((terms, LANES), 1) // vectors
    left = lambda a: pltpu.roll(a, LANES - vectors, 1)
    right = lambda a: pltpu.roll(a, vectors, 1)
    w = jnp.where(quarter == 1, left(w), jnp.where(quarter == 2, right(w), w))
    x = jnp.where(quarter == 0, right(x), jnp.where(quarter == 3, left(x), x))
    w = jnp.where((quarter == 1) | (quarter == 3), -w, w)
    fields = w + jnp.where(quarter >= 2, -x, x)
    front = iota((orders, LANES), 1) < LANES // 2
    for pair in range(live // 2):
        a = fields[2 * pair * orders : (2 * pair + 1) * orders]
        b = fields[(2 * pair + 1) * orders : (2 * pair + 2) * orders]
        both = jnp.concatenate([jnp.where(front, a, swap(b)), jnp.where(front, swap(a), b)], axis=0)
        message[:, pair * LANES : (pair + 1) * LANES] = both.astype(BF16)

    def ma_copy(kind, source, target, slot, peer):
        return pltpu.make_async_remote_copy(
            src_ref=source,
            dst_ref=target.at[slot],
            send_sem=ma_send.at[kind, peer],
            recv_sem=ma_recv.at[kind, slot],
            device_id=(peer, vert),
            device_id_type=MESH,
        )

    def over_ma(act):
        def body(step, carry):
            act(ma_peer(step))
            return carry

        lax.fori_loop(1, n_ma, body, 0)

    def ma_start(kind, source, target):
        over_ma(lambda peer: ma_copy(kind, source, target, ma, peer).start())

    def ma_wait(kind, source, target):
        over_ma(lambda peer: ma_copy(kind, source, target, peer, peer).wait_recv())

    def ma_done(kind, source, target):
        over_ma(lambda peer: ma_copy(kind, source, target, ma, peer).wait_send())

    def vert_copy(kind, source, target, slot, peer):
        return pltpu.make_async_remote_copy(
            src_ref=source,
            dst_ref=target.at[slot],
            send_sem=vert_send.at[kind, peer],
            recv_sem=vert_recv.at[kind, slot],
            device_id=(ma, peer),
            device_id_type=MESH,
        )

    def over_vert(act):
        def body(step, carry):
            act(vert_peer(step))
            return carry

        lax.fori_loop(1, n_vert, body, 0)

    def vert_start(kind, source, target):
        over_vert(lambda peer: vert_copy(kind, source, target, vert, peer).start())

    def vert_wait(kind, source, target):
        over_vert(lambda peer: vert_copy(kind, source, target, peer, peer).wait_recv())

    def vert_done(kind, source, target):
        over_vert(lambda peer: vert_copy(kind, source, target, vert, peer).wait_send())

    ma_start(0, message, gathered)
    gathered[ma] = message[...]

    turned = spectra[...].T
    part = [turned[c * vectors : (c + 1) * vectors] for c in range(parts)]
    wide = part[0].shape
    sign = half_sign(wide, 1.0, -1.0)
    field_x = (part[0] + swap(part[3])) * sign
    field_y = part[1] - swap(part[2])
    for n, (piece_x, piece_y) in enumerate(zip(split(field_x, 3), split(field_y, 3))):
        at = slice((3 + n) * vectors, (4 + n) * vectors)
        lhs[at, : 2 * terms] = piece_x
        lhs[at, 2 * terms :] = piece_y

    step_rows = min(2 * terms, LANES)

    def leg_products(i, carry):
        at = rows_at(i, step_rows)
        found = mm_nt(leg_ref[at, :], leg_ref[...])
        same = lax.rem(iota(found.shape, 0) - iota(found.shape, 1) + 2 * terms * orders, orders) == 0
        for n, piece in enumerate(split(jnp.where(same, found, 0.0), 3)):
            llm[n, at, :] = piece
        return carry

    lax.fori_loop(0, 2 * terms // step_rows, leg_products, 0)

    scale = 1.0 / math.sqrt(n_ma * orders)
    width = n_ma * 2 * orders
    lane = iota((8, width), 1)
    slot = lane // (2 * orders) * orders + lax.rem(lane, orders)

    def place_order(i, carry):
        return jnp.where(slot == i, order_ref[i], carry)

    lane_order = lax.fori_loop(0, n_ma * orders, place_order, jnp.zeros((8, width), I32))
    shift = jnp.where(lax.rem(lane // orders, 2) == 1, longitudes - longitudes // 4, 0)

    def table_rows(i, carry):
        j = iota((LANES, width), 0) + i * LANES
        phase = modulo(j * lane_order[:1] + shift[:1], longitudes)
        tables[rows_at(i, LANES), :] = (cosines(phase, longitudes) * scale).astype(BF16)
        return carry

    lax.fori_loop(0, longitudes // LANES, table_rows, 0)
    row = iota((2 * orders, longitudes), 0)
    own_order = jnp.zeros((2 * orders, longitudes), I32)
    for s in range(orders):
        own_order = jnp.where(lax.rem(row, orders) == s, order_ref[ma * orders + s], own_order)
    phase = iota((2 * orders, longitudes), 1) * own_order
    phase = phase + jnp.where(row >= orders, longitudes - longitudes // 4, 0)
    back_table[...] = (cosines(modulo(phase, longitudes), longitudes) * scale).astype(BF16)

    ma_wait(0, message, gathered)
    columns = message.shape[1]
    wide_block = min(columns, 512)
    cycles_here = wide_block // (2 * vectors)

    def transform(block, carry):
        at = rows_at(block, wide_block)
        grid = mm(tables[...], gathered[:, :, at].reshape(n_ma * 2 * orders, wide_block))
        lane_cycle = iota((8, wide_block), 1) // (2 * vectors)
        begin = jnp.zeros((8, wide_block), I32)
        length = jnp.zeros((8, wide_block), I32)
        weight = jnp.zeros((8, wide_block), F32)
        for r in range(cycles_here):
            here = lane_cycle == r
            cycle = first + block * cycles_here + r
            begin = jnp.where(here, start_ref[cycle], begin)
            length = jnp.where(here, count_ref[cycle], length)
            weight = jnp.where(here, weight_ref[cycle], weight)
        away = iota(grid.shape, 0) - begin[:1]
        away = jnp.where(away < 0, away + longitudes, away)
        weighted = (grid * jnp.where(away < length[:1], weight[:1], 0.0)).astype(BF16)
        found = mm(back_table[...], weighted)
        for n in range(wide_block // LANES):
            both = found[:, n * LANES : (n + 1) * LANES]
            c, s = both[:orders], both[orders:]
            pair = [jnp.where(front, c, swap(s)), jnp.where(front, swap(c), s)]
            for e in range(2):
                cycle = block * cycles_here + 2 * n + e
                returned[rows_at(cycle, orders), :] = pair[e]
        return carry

    lax.fori_loop(0, columns // wide_block, transform, 0)
    here = returned[...]
    even = lax.rem(iota(here.shape, 1) // vectors, 2) == 0
    turned = jnp.concatenate([here, jnp.where(even, right(here), left(here))], axis=0).T
    turned = turned.astype(BF16)
    g_x = turned[:vectors]
    back_y = turned[vectors : 2 * vectors]
    g_y = turned[2 * vectors : 3 * vectors]
    back_x = turned[3 * vectors :]
    packed[vert, :, : 2 * terms] = g_x
    packed[vert, :, 2 * terms :] = g_y
    vert_start(0, packed.at[vert], packed)
    send_far(cuts[0], cuts[1])

    signs = sign.astype(BF16)
    adjoint = jnp.concatenate([g_x * signs, g_y, -back_y, -back_x * signs], axis=0)
    products = mm(adjoint, llm[0]) + mm(adjoint, llm[1]) + mm(adjoint, llm[2])
    part = [products[c * vectors : (c + 1) * vectors] for c in range(parts)]
    gram_x = part[0] * sign + swap(part[3] * -sign)
    gram_y = part[1] - swap(part[2])
    for n, (piece_x, piece_y) in enumerate(zip(split(gram_x, 3), split(gram_y, 3))):
        at = slice(n * vectors, (n + 1) * vectors)
        lhs[at, : 2 * terms] = piece_x
        lhs[at, 2 * terms :] = piece_y

    vert_wait(0, packed.at[vert], packed)
    everyone = packed[...].reshape(total, 4 * terms)
    found = mm_nt(lhs[...], everyone)
    found = [found[n * vectors : (n + 1) * vectors] for n in range(6)]
    row_a[...] = found[0] + found[1] + found[2]
    ma_start(1, row_a, land_a)
    land_a[ma] = row_a[...]
    row_b[...] = found[3] + found[4] + found[5]
    land_b[ma] = row_b[...]

    for i in range(n_vert):
        near_copy(i, 1 - place).wait_recv()
    wide = parts * vectors
    near_sums = jnp.zeros((wide, 2 * wide), F32)
    for i in range(n_vert):
        for e in range(share):
            here = mine[i, e].reshape(wide, degrees)
            both = jnp.concatenate([here, theirs[pair_at(i), e].reshape(wide, degrees)], axis=0)
            near_sums = near_sums + mm_nt(here, both)
    first_half, second_half = [
        sum(
            near_sums[c * vectors : (c + 1) * vectors, n * wide + c * vectors : n * wide + (c + 1) * vectors]
            for c in range(parts)
        )
        for n in range(2)
    ]
    near_sums = jnp.concatenate([first_half, second_half], axis=1)
    swapped = jnp.concatenate([second_half, first_half], axis=1)
    near_sums = jnp.where(place == 0, near_sums, swapped)
    row_e[...] = jnp.concatenate([near_sums[: vectors // 2], near_sums[vectors // 2 :]], axis=1)
    ma_start(4, row_e, land_e)
    land_e[ma] = row_e[...]

    ma_wait(1, row_a, land_a)
    sum_a[vert] = jnp.sum(land_a[...], axis=0)
    vert_start(1, sum_a.at[vert], sum_a)
    send_far(cuts[1], cuts[2])
    ma_start(2, row_b, land_b)
    ma_wait(4, row_e, land_e)
    sum_e[vert] = jnp.sum(land_e[...], axis=0)
    vert_start(4, sum_e.at[vert], sum_e)
    send_far(cuts[2], pieces)

    vert_wait(1, sum_a.at[vert], sum_a)
    inverse_count = 1.0 / (n_ma * orders * parts * degrees)
    work[:, :total] = sum_a[...].reshape(total, total) * inverse_count
    work[:, total:] = (iota((total, total), 0) == iota((total, total), 1)).astype(F32)

    def panel_step(p, carry):
        factor_panel(work, p)
        return carry

    panels = total // PANEL
    lax.fori_loop(0, panels // 2, panel_step, 0)

    ma_wait(2, row_b, land_b)
    sum_b[vert] = jnp.sum(land_b[...], axis=0)

    def far_wait(piece, carry):
        far_copy(piece, True).wait_recv()
        return carry

    lax.fori_loop(0, pieces, far_wait, 0)

    cross_sums = jnp.zeros((2 * wide, 2 * wide), F32)
    for e in range(share):
        here = [mine[half, e].reshape(wide, degrees), theirs[vert, e].reshape(wide, degrees)]
        there = far[:, e].reshape(half * wide, degrees)
        cross_sums = cross_sums + mm_nt(jnp.concatenate(here, axis=0), there)
    cross_sums = jnp.concatenate(
        [
            jnp.concatenate(
                [
                    sum(
                        cross_sums[
                            m * wide + c * vectors : m * wide + (c + 1) * vectors,
                            n * wide + c * vectors : n * wide + (c + 1) * vectors,
                        ]
                        for c in range(parts)
                    )
                    for n in range(2)
                ],
                axis=1,
            )
            for m in range(2)
        ],
        axis=0,
    )
    swapped = jnp.concatenate([cross_sums[vectors:], cross_sums[:vectors]], axis=0)
    cross_sums = jnp.where(place == 0, cross_sums, swapped)
    cross_sums = jnp.where(side == 0, cross_sums, cross_sums.T)
    size = half * vectors
    ab_own[...] = jnp.concatenate([cross_sums[: size // 2], cross_sums[size // 2 :]], axis=1)
    vert_start(3, ab_own, land_c)
    land_c[vert] = ab_own[...]

    vert_wait(4, sum_e.at[vert], sum_e)
    blocks = sum_e[...]
    size = half * vectors
    near_blocks = [
        jnp.concatenate([blocks[n][:, :size], blocks[n][:, size:]], axis=0) * inverse_count
        for n in range(n_vert)
    ]
    diagonals = [jnp.concatenate(near_blocks[n * half : (n + 1) * half], axis=0) for n in range(2)]
    unit = (iota((size, size), 0) == iota((size, size), 1)).astype(F32)
    corner[...] = jnp.concatenate([diagonals[0], unit], axis=1)

    def both_step(p, carry):
        factor_panel(work, panels // 2 + p)
        factor_panel(corner, p)
        return carry

    lax.fori_loop(0, panels // 2, both_step, 0)
    in_front = iota(corner.shape, 1) < size
    inverse = jnp.where(in_front, swap(corner[...]), 0.0)
    corner_ref[...] = jnp.concatenate([inverse[:, :size], diagonals[1]], axis=1)

    vert_wait(3, ab_own, land_c)
    ab_mid[...] = jnp.sum(land_c[...], axis=0)
    ma_start(3, ab_mid, land_d)
    land_d[ma] = ab_mid[...]
    vert_start(2, sum_b.at[vert], sum_b)

    mixing = work[rows_at(vert, vectors), total:].astype(BF16)
    spread = (iota((parts * vectors, vectors), 0) // parts == iota((parts * vectors, vectors), 1))
    mixing = mm(spread.astype(BF16), mixing).astype(BF16)
    mixed = mm(mixing, everyone)
    mixed_x, mixed_y = mixed[:, : 2 * terms], mixed[:, 2 * terms :]
    kind = lax.rem(iota(mixed_x.shape, 0), parts)
    sign = half_sign(mixed_x.shape, 1.0, -1.0)
    mixer = jnp.where(
        kind == 0, mixed_x * sign,
        jnp.where(kind == 1, mixed_y, jnp.where(kind == 2, -swap(mixed_y), -swap(mixed_x) * sign)),
    )
    pieces_of = split(mixer, 2)
    lane_order = modulo(iota(mixer.shape, 1), orders)

    def mix(s, carry):
        chosen = [jnp.where(lane_order == s, piece, jnp.zeros_like(piece)) for piece in pieces_of]
        mixed = mm(chosen[0], leg_ref[...]) + mm(chosen[1], leg_ref[...])
        basis_ref[:, s] = mixed.reshape(vectors, parts, degrees).astype(BF16)
        return carry

    lax.fori_loop(0, orders, mix, 0)

    vert_wait(2, sum_b.at[vert], sum_b)
    lower = (iota((size, total), 0) + size == iota((size, total), 1)).astype(F32)
    outer = jnp.concatenate([inverse, lower], axis=0)
    crossed = jnp.dot(
        outer, sum_b[...].reshape(total, total) * inverse_count,
        precision=HIGHEST, preferred_element_type=F32,
    )
    cross_ref[...] = lax.dot_general(
        crossed, outer, NT, precision=HIGHEST, preferred_element_type=F32
    )
    ma_wait(3, ab_mid, land_d)
    ab_ref[...] = jnp.sum(land_d[...], axis=0) * inverse_count

    for i in range(n_vert):
        near_copy(i, place).wait_send()

    def far_done(piece, carry):
        far_copy(piece).wait_send()
        return carry

    lax.fori_loop(0, pieces, far_done, 0)
    ma_done(0, message, gathered)
    vert_done(0, packed.at[vert], packed)
    ma_done(1, row_a, land_a)
    ma_done(2, row_b, land_b)
    vert_done(1, sum_a.at[vert], sum_a)
    vert_done(2, sum_b.at[vert], sum_b)
    ma_done(4, row_e, land_e)
    vert_done(4, sum_e.at[vert], sum_e)
    vert_done(3, ab_own, land_c)
    ma_done(3, ab_mid, land_d)


def step_terms(trial, legendre, order_slot, cycle_start, cycle_count, cycle_weight, n_ma, n_vert):
    vectors, orders, per, _ = trial.shape
    _, kinds, cycles, degrees = legendre.shape
    parts = per * LANES // degrees
    live = cycles // 4
    terms = live * orders
    total = n_vert * vectors
    half = n_vert // 2
    share = orders // n_vert
    longitudes = 2 * n_ma * orders
    pieces = half * share * parts
    columns = live * 2 * vectors
    grant = min(60, 16 + terms // 16) * MIB
    anywhere = pl.BlockSpec(memory_space=pltpu.HBM)
    return pl.pallas_call(
        functools.partial(step_kernel, n_ma, n_vert, live),
        out_shape=(
            jax.ShapeDtypeStruct((total, total), F32),
            jax.ShapeDtypeStruct((half * vectors, 2 * half * vectors), F32),
            jax.ShapeDtypeStruct((half * vectors // 2, 2 * half * vectors), F32),
            jax.ShapeDtypeStruct((vectors, orders, parts, degrees), BF16),
        ),
        in_specs=[anywhere] * 6,
        out_specs=[pl.BlockSpec(memory_space=VMEM)] * 4,
        scratch_shapes=[
            VMEM((2 * terms, degrees), BF16),
            VMEM((n_vert, vectors, share, per, LANES), BF16),
            VMEM(legendre.shape, BF16),
            VMEM((n_vert, share, parts, vectors, degrees), BF16),
            VMEM((n_vert, share, parts, vectors, degrees), BF16),
            VMEM((half, share, parts, vectors, degrees), BF16),
            VMEM((2 * orders, columns), BF16),
            VMEM((n_ma, 2 * orders, columns), BF16),
            VMEM((2 * terms, LANES), F32),
            VMEM((terms, LANES), F32),
            VMEM((n_vert, vectors, 4 * terms), BF16),
            VMEM((vectors, total), F32),
            VMEM((n_ma, vectors, total), F32),
            VMEM((n_vert, vectors, total), F32),
            VMEM((vectors, total), F32),
            VMEM((n_ma, vectors, total), F32),
            VMEM((n_vert, vectors, total), F32),
            VMEM((vectors // 2, 2 * half * vectors), F32),
            VMEM((n_ma, vectors // 2, 2 * half * vectors), F32),
            VMEM((n_vert, vectors // 2, 2 * half * vectors), F32),
            VMEM((half * vectors // 2, 2 * half * vectors), F32),
            VMEM((n_vert, half * vectors // 2, 2 * half * vectors), F32),
            VMEM((half * vectors // 2, 2 * half * vectors), F32),
            VMEM((n_ma, half * vectors // 2, 2 * half * vectors), F32),
            VMEM((total, 2 * total), F32),
            VMEM((half * vectors, 2 * half * vectors), F32),
            VMEM((6 * vectors, 4 * terms), BF16),
            VMEM((3, 2 * terms, 2 * terms), BF16),
            VMEM((longitudes, n_ma * 2 * orders), BF16),
            VMEM((2 * orders, longitudes), BF16),
            SMEM(order_slot.shape, I32),
            SMEM(cycle_start.shape, I32),
            SMEM(cycle_count.shape, I32),
            SMEM(cycle_weight.shape, F32),
            DMA((n_vert,)),
            DMA,
            DMA((4,)),
            DMA((n_vert,)),
            DMA((n_vert,)),
            DMA((pieces,)),
            DMA((pieces,)),
            DMA((5, n_ma)),
            DMA((5, n_ma)),
            DMA((5, n_vert)),
            DMA((5, n_vert)),
        ],
        compiler_params=pltpu.CompilerParams(
            collective_id=0, has_side_effects=True, vmem_limit_bytes=grant
        ),
        name="step_terms",
    )(trial, legendre, order_slot, cycle_start, cycle_count, cycle_weight)


def finish_kernel(cross_ref, corner_ref, ab_ref, staged_ref, basis_ref, ritz_ref, work, sem):
    total = ritz_ref.shape[0]
    size = total // 2
    out = pltpu.make_async_copy(staged_ref, basis_ref, sem)
    out.start()
    ab = ab_ref[...]
    ab = jnp.concatenate([ab[:, :size], ab[:, size:]], axis=0)
    inverse, diagonal = corner_ref[:, :size], corner_ref[:, size:]
    beside = jnp.dot(inverse, ab, precision=HIGHEST, preferred_element_type=F32)
    taken = lax.dot_general(
        beside, beside, (((0,), (0,)), ((), ())), precision=HIGHEST, preferred_element_type=F32
    )
    unit = (iota((size, size), 0) == iota((size, size), 1)).astype(F32)
    work[:, :total] = jnp.concatenate([diagonal - taken, jnp.zeros_like(unit)], axis=1)
    work[:, total:] = jnp.concatenate([-beside.T, unit], axis=1)

    def step(p, carry):
        factor_panel(work, p)
        return carry

    lax.fori_loop(0, size // PANEL, step, 0)
    upper = (iota((size, total), 0) == iota((size, total), 1)).astype(F32)
    outer = jnp.concatenate([upper, work[:, total:]], axis=0)
    crossed = jnp.dot(outer, cross_ref[...], precision=HIGHEST, preferred_element_type=F32)
    ritz_ref[...] = lax.dot_general(
        crossed, outer, NT, precision=HIGHEST, preferred_element_type=F32
    )
    out.wait()


def finish(cross, corner, ab, staged):
    total = cross.shape[0]
    return pl.pallas_call(
        finish_kernel,
        out_shape=(
            jax.ShapeDtypeStruct(staged.shape, BF16),
            jax.ShapeDtypeStruct((total, total), F32),
        ),
        in_specs=[pl.BlockSpec(memory_space=VMEM)] * 4,
        out_specs=(pl.BlockSpec(memory_space=pl.ANY), pl.BlockSpec(memory_space=VMEM)),
        scratch_shapes=[VMEM((total // 2, 2 * total), F32), DMA],
        compiler_params=pltpu.CompilerParams(vmem_limit_bytes=8 * MIB),
        name="finish",
    )(cross, corner, ab, staged)


def shards(trial_block, legendre, order_slot, cycle_start, cycle_count, cycle_weight):
    n_ma = lax.axis_size("ma")
    n_vert = lax.axis_size("vert")
    vectors, orders, parts, degrees = trial_block.shape
    trial = trial_block.reshape(vectors, orders, parts, degrees // LANES, LANES)
    trial = trial.transpose(0, 1, 3, 2, 4).reshape(vectors, orders, parts * degrees // LANES, LANES)
    inputs = (trial, legendre, order_slot, cycle_start, cycle_count, cycle_weight)
    inputs = [pltpu.with_memory_space_constraint(x, pltpu.HBM) for x in inputs]
    return finish(*step_terms(*inputs, n_ma, n_vert))


def solution(mesh):
    in_specs = (P("vert", "ma", None, None), P("ma", None, None, None), P(), P(), P(), P())
    out_specs = (P("vert", "ma", None, None), P())
    return jax.shard_map(shards, mesh=mesh, in_specs=in_specs, out_specs=out_specs, check_vma=False)
```

```python
import functools
import math

import jax
import jax.numpy as jnp
from jax import lax
from jax.experimental import pallas as pl
from jax.experimental.pallas import tpu as pltpu
from jax.sharding import PartitionSpec as P

MESH = pl.DeviceIdType.MESH
VMEM = pltpu.VMEM
SMEM = pltpu.SMEM
DMA = pltpu.SemaphoreType.DMA
F32 = jnp.float32
BF16 = jnp.bfloat16
I32 = jnp.int32
HIGHEST = lax.Precision.HIGHEST
MIB = 1024 * 1024
LANES = 128
PANEL = 16
NT = (((1,), (1,)), ((), ()))
STAGES = (6, 13, 14)


def iota(shape, axis):
    return lax.broadcasted_iota(I32, shape, axis)


def mm(a, b):
    return jnp.dot(a, b, preferred_element_type=F32)


def mm_nt(a, b):
    return lax.dot_general(a, b, NT, preferred_element_type=F32)


def split(x, count):
    pieces = []
    for _ in range(count):
        piece = x.astype(BF16)
        pieces.append(piece)
        x = x - piece.astype(F32)
    return pieces


def stacked(x, axis, first):
    high, middle, low = split(x, 3)
    order = (high, high, high, middle, middle, low) if first else (high, middle, low, high, middle, high)
    return jnp.concatenate(order, axis=axis)


def fine(a, b, a_axis, b_axis):
    dims = (((a_axis,), (b_axis,)), ((), ()))
    a, b = stacked(a, a_axis, True), stacked(b, b_axis, False)
    return lax.dot_general(a, b, dims, preferred_element_type=F32)


def swap(x):
    return pltpu.roll(x, x.shape[1] // 2, 1)


def half_sign(shape, first, second):
    return jnp.where(iota(shape, 1) < shape[1] // 2, first, second).astype(F32)


def rows_at(index, count):
    return pl.ds(pl.multiple_of(index * count, count), count)


def factor_panel(work, p):
    size, width = work.shape
    first = pl.multiple_of(p * PANEL, PANEL)
    at = pl.ds(first, PANEL)
    lane = iota((PANEL, size), 1)
    sub = iota((PANEL, width), 0)
    x = work[at, :]
    column = [
        jnp.sum(jnp.where(lane == first + i, x[:, :size], 0.0), axis=1, keepdims=True)
        for i in range(PANEL)
    ]
    for i in range(PANEL):
        inverse = lax.rsqrt(column[i][i : i + 1, :])
        scaled = column[i] * inverse
        for k in range(i + 1, PANEL):
            column[k] = column[k] - scaled * (column[k][i : i + 1, :] * inverse)
        line = x[i : i + 1, :] * inverse
        x = jnp.where(sub == i, line, jnp.where(sub > i, x - scaled * line, x))
    high, middle, low = split(x, 3)
    left = jnp.concatenate([high, high, high, middle, middle, low], axis=0)
    right = jnp.concatenate([high, middle, low, high, middle, high], axis=0)
    update = lax.dot_general(
        left[:, :size], right, (((0,), (0,)), ((), ())), preferred_element_type=F32
    )
    below = iota((size, width), 0) >= first + PANEL
    work[...] = jnp.where(below, work[...] - update, work[...])
    work[at, :] = x


def cosines(phase, total):
    phase = jnp.where(phase > total // 2, total - phase, phase)
    turned = phase > total // 4
    x = jnp.where(turned, total // 2 - phase, phase).astype(F32) * (2.0 * math.pi / total)
    y = x * x
    value = jnp.full_like(y, 1.0 / math.factorial(12))
    for n in (10, 8, 6, 4, 2, 0):
        value = value * y * (1.0 if n % 4 == 2 else 1.0) + (-1.0) ** (n // 2) / math.factorial(n)
    return jnp.where(turned, -value, value)


def modulo(x, total):
    return x & (total - 1) if total & (total - 1) == 0 else lax.rem(x, total)


def step_kernel(
    n_ma, n_vert, live,
    trial_ref, legendre_ref, order_in, start_in, count_in, weight_in,
    cross_ref, corner_ref, ab_ref, basis_ref,
    leg_ref, native, leg_in, mine, theirs, far, message, gathered, spectra, returned, packed,
    row_a, land_a, sum_a, row_b, land_b, sum_b, row_e, land_e, sum_e, ab_own, land_c, ab_mid, land_d,
    work, corner, lhs, llm, tables, back_table,
    order_ref, start_ref, count_ref, weight_ref,
    load_sem, leg_sem, small_sem, near_send, near_recv, far_send, far_recv,
    ma_send, ma_recv, vert_send, vert_recv,
):
    ma = lax.axis_index("ma")
    vert = lax.axis_index("vert")
    _, vectors, share, per, _ = native.shape
    orders = n_vert * share
    parts, degrees = mine.shape[2], mine.shape[4]
    tiles = degrees // LANES
    cycles = leg_in.shape[2]
    half = n_vert // 2
    place = lax.rem(vert, half)
    side = vert // half
    assert half == 2
    total = n_vert * vectors
    terms = live * orders
    longitudes = 2 * n_ma * orders

    barrier = pltpu.get_barrier_semaphore()

    def ma_peer(step):
        return lax.rem(ma + step, n_ma)

    def vert_peer(step):
        return lax.rem(vert + step, n_vert)

    def greet_ma(step, carry):
        pl.semaphore_signal(barrier, inc=1, device_id=(ma_peer(step), vert), device_id_type=MESH)
        return carry

    def greet_vert(step, carry):
        pl.semaphore_signal(barrier, inc=1, device_id=(ma, vert_peer(step)), device_id_type=MESH)
        return carry

    lax.fori_loop(1, n_ma, greet_ma, 0)
    lax.fori_loop(1, n_vert, greet_vert, 0)

    def pair_at(i, place=place):
        group = 1 - side if i < half else side
        return group * half + lax.rem(place + i, half)

    def load(i):
        at = pl.ds(pair_at(i) * share, share)
        return pltpu.make_async_copy(trial_ref.at[:, at], native.at[i], load_sem.at[i])

    leg_copy = pltpu.make_async_copy(legendre_ref, leg_in, leg_sem)
    small = [(order_in, order_ref), (start_in, start_ref), (count_in, count_ref), (weight_in, weight_ref)]
    small = [pltpu.make_async_copy(*pair, small_sem.at[n]) for n, pair in enumerate(small)]
    for copy in small:
        copy.start()
    for i in range(n_vert):
        load(i).start()
        if i == half - 1:
            leg_copy.start()

    rows = 8 * per
    row = iota((rows, rows), 0)
    column = iota((rows, rows), 1)
    wanted = modulo(row, 8) * per + modulo(row // 8, tiles) * parts + row // (8 * tiles)
    reorder = (column == wanted).astype(BF16)

    def arrange(i):
        load(i).wait()
        for g in range(vectors // 16):
            for e in range(0, share, 2):
                blocks = []
                for h in range(2):
                    at = pl.ds(16 * g + 8 * h, 8)
                    both = [native[i, at, e + n].reshape(rows, LANES) for n in range(2)]
                    blocks.append(mm(reorder, jnp.concatenate(both, axis=1)))
                for n in range(2):
                    for c in range(parts):
                        for t in range(tiles):
                            lo = (c * tiles + t) * 8
                            at = (slice(lo, lo + 8), slice(n * LANES, (n + 1) * LANES))
                            tile = jnp.concatenate([blocks[0][at], blocks[1][at]], axis=0)
                            at = (slice(16 * g, 16 * g + 16), slice(t * LANES, (t + 1) * LANES))
                            mine[(i, e + n, c) + at] = tile.astype(BF16)

    def near_copy(i, source):
        return pltpu.make_async_remote_copy(
            src_ref=mine.at[i],
            dst_ref=theirs.at[pair_at(i, source)],
            send_sem=near_send.at[i],
            recv_sem=near_recv.at[i],
            device_id=(ma, side * half + 1 - place),
            device_id_type=MESH,
        )

    each = share * parts
    pieces = half * each

    def far_copy(piece, arriving=False):
        offset = piece // each
        inner = lax.rem(piece, each)
        peer = (1 - side) * half + lax.rem(place + offset, half)
        slot = lax.rem(place + half - offset, half) if arriving else place
        s = inner // parts
        c = lax.rem(inner, parts)
        return pltpu.make_async_remote_copy(
            src_ref=mine.at[offset, s, c],
            dst_ref=far.at[slot, s, c],
            send_sem=far_send.at[piece],
            recv_sem=far_recv.at[piece],
            device_id=(ma, peer),
            device_id_type=MESH,
        )

    def send_far(begin, end):
        def body(piece, carry):
            far_copy(piece).start()
            return carry

        lax.fori_loop(begin, end, body, 0)

    cuts = [min(pieces, cut) for cut in STAGES]
    arrange(0)
    pl.semaphore_wait(barrier, n_ma + n_vert - 2)
    send_far(0, min(each, cuts[0]))
    for i in range(1, half):
        arrange(i)
    if cuts[0] > each:
        send_far(each, cuts[0])

    for copy in small:
        copy.wait()

    def search(i, found):
        j = cycles - 1 - i
        return jnp.where(count_ref[j] > 0, j, found)

    first = jnp.minimum(lax.fori_loop(0, cycles, search, 0), cycles - live)

    leg_copy.wait()
    block = min(terms, 64)
    for kind in range(2):
        source = leg_in[:, kind].reshape(orders * cycles, degrees)

        def pick(i, carry):
            row = iota((block, orders * cycles), 0) + i * block
            column = iota((block, orders * cycles), 1)
            wanted = modulo(row, orders) * cycles + row // orders + first
            at = rows_at(kind * (terms // block) + i, block)
            leg_ref[at, :] = mm((column == wanted).astype(BF16), source).astype(BF16)
            return carry

        lax.fori_loop(0, terms // block, pick, 0)

    for i in range(half, n_vert):
        arrange(i)
    for i in range(n_vert):
        near_copy(i, place).start()

    keep = lax.rem(iota((2 * terms, LANES), 0), orders)

    for i in range(n_vert):
        both = mm_nt(leg_ref[...], mine[i].reshape(share * parts * vectors, degrees))
        for e in range(share):
            found = both[:, e * LANES : (e + 1) * LANES]
            here = keep == pair_at(i) * share + e
            spectra[...] = jnp.where(here, found, spectra[...]) if i + e else found
    w = spectra[:terms, :]
    x = spectra[terms:, :]
    quarter = iota((terms, LANES), 1) // vectors
    left = lambda a: pltpu.roll(a, LANES - vectors, 1)
    right = lambda a: pltpu.roll(a, vectors, 1)
    w = jnp.where(quarter == 1, left(w), jnp.where(quarter == 2, right(w), w))
    x = jnp.where(quarter == 0, right(x), jnp.where(quarter == 3, left(x), x))
    w = jnp.where((quarter == 1) | (quarter == 3), -w, w)
    fields = w + jnp.where(quarter >= 2, -x, x)
    front = iota((orders, LANES), 1) < LANES // 2
    for pair in range(live // 2):
        a = fields[2 * pair * orders : (2 * pair + 1) * orders]
        b = fields[(2 * pair + 1) * orders : (2 * pair + 2) * orders]
        both = jnp.concatenate([jnp.where(front, a, swap(b)), jnp.where(front, swap(a), b)], axis=0)
        message[:, pair * LANES : (pair + 1) * LANES] = both.astype(BF16)

    def ma_copy(kind, source, target, slot, peer):
        return pltpu.make_async_remote_copy(
            src_ref=source,
            dst_ref=target.at[slot],
            send_sem=ma_send.at[kind, peer],
            recv_sem=ma_recv.at[kind, slot],
            device_id=(peer, vert),
            device_id_type=MESH,
        )

    def over_ma(act):
        def body(step, carry):
            act(ma_peer(step))
            return carry

        lax.fori_loop(1, n_ma, body, 0)

    def ma_start(kind, source, target):
        over_ma(lambda peer: ma_copy(kind, source, target, ma, peer).start())

    def ma_wait(kind, source, target):
        over_ma(lambda peer: ma_copy(kind, source, target, peer, peer).wait_recv())

    def ma_done(kind, source, target):
        over_ma(lambda peer: ma_copy(kind, source, target, ma, peer).wait_send())

    def vert_copy(kind, source, target, slot, peer):
        return pltpu.make_async_remote_copy(
            src_ref=source,
            dst_ref=target.at[slot],
            send_sem=vert_send.at[kind, peer],
            recv_sem=vert_recv.at[kind, slot],
            device_id=(ma, peer),
            device_id_type=MESH,
        )

    def over_vert(act):
        def body(step, carry):
            act(vert_peer(step))
            return carry

        lax.fori_loop(1, n_vert, body, 0)

    def vert_start(kind, source, target):
        over_vert(lambda peer: vert_copy(kind, source, target, vert, peer).start())

    def vert_wait(kind, source, target):
        over_vert(lambda peer: vert_copy(kind, source, target, peer, peer).wait_recv())

    def vert_done(kind, source, target):
        over_vert(lambda peer: vert_copy(kind, source, target, vert, peer).wait_send())

    beside = side * half + 1 - place
    across = (1 - side) * half + place
    last = (1 - side) * half + 1 - place

    def hand_over(kind, target, slot, key):
        return pltpu.make_async_remote_copy(
            src_ref=target.at[slot],
            dst_ref=target.at[slot],
            send_sem=vert_send.at[kind, key],
            recv_sem=vert_recv.at[kind, slot],
            device_id=(ma, beside),
            device_id_type=MESH,
        )

    def gather_start(kind, target):
        vert_copy(kind, target.at[vert], target, vert, across).start()
        vert_copy(kind, target.at[vert], target, vert, beside).start()

    def gather_wait(kind, target):
        vert_copy(kind, target.at[vert], target, across, across).wait_recv()
        hand_over(kind, target, across, last).start()
        vert_copy(kind, target.at[vert], target, beside, beside).wait_recv()
        vert_copy(kind, target.at[vert], target, last, last).wait_recv()

    def gather_done(kind, target):
        vert_copy(kind, target.at[vert], target, vert, across).wait_send()
        vert_copy(kind, target.at[vert], target, vert, beside).wait_send()
        hand_over(kind, target, across, last).wait_send()

    ma_start(0, message, gathered)
    gathered[ma] = message[...]

    turned = spectra[...].T
    part = [turned[c * vectors : (c + 1) * vectors] for c in range(parts)]
    wide = part[0].shape
    sign = half_sign(wide, 1.0, -1.0)
    field_x = (part[0] + swap(part[3])) * sign
    field_y = part[1] - swap(part[2])
    for n, (piece_x, piece_y) in enumerate(zip(split(field_x, 3), split(field_y, 3))):
        at = slice((3 + n) * vectors, (4 + n) * vectors)
        lhs[at, : 2 * terms] = piece_x
        lhs[at, 2 * terms :] = piece_y

    step_rows = min(2 * terms, LANES)

    def leg_products(i, carry):
        at = rows_at(i, step_rows)
        found = mm_nt(leg_ref[at, :], leg_ref[...])
        same = lax.rem(iota(found.shape, 0) - iota(found.shape, 1) + 2 * terms * orders, orders) == 0
        for n, piece in enumerate(split(jnp.where(same, found, 0.0), 3)):
            llm[n, at, :] = piece
        return carry

    lax.fori_loop(0, 2 * terms // step_rows, leg_products, 0)

    scale = 1.0 / math.sqrt(n_ma * orders)
    width = n_ma * 2 * orders
    lane = iota((8, width), 1)
    slot = lane // (2 * orders) * orders + lax.rem(lane, orders)

    def place_order(i, carry):
        return jnp.where(slot == i, order_ref[i], carry)

    lane_order = lax.fori_loop(0, n_ma * orders, place_order, jnp.zeros((8, width), I32))
    shift = jnp.where(lax.rem(lane // orders, 2) == 1, longitudes - longitudes // 4, 0)

    def table_rows(i, carry):
        j = iota((LANES, width), 0) + i * LANES
        phase = modulo(j * lane_order[:1] + shift[:1], longitudes)
        tables[rows_at(i, LANES), :] = (cosines(phase, longitudes) * scale).astype(BF16)
        return carry

    lax.fori_loop(0, longitudes // LANES, table_rows, 0)
    row = iota((2 * orders, longitudes), 0)
    own_order = jnp.zeros((2 * orders, longitudes), I32)
    for s in range(orders):
        own_order = jnp.where(lax.rem(row, orders) == s, order_ref[ma * orders + s], own_order)
    phase = iota((2 * orders, longitudes), 1) * own_order
    phase = phase + jnp.where(row >= orders, longitudes - longitudes // 4, 0)
    back_table[...] = (cosines(modulo(phase, longitudes), longitudes) * scale).astype(BF16)

    ma_wait(0, message, gathered)
    columns = message.shape[1]
    wide_block = min(columns, 512)
    cycles_here = wide_block // (2 * vectors)

    def transform(block, carry):
        at = rows_at(block, wide_block)
        grid = mm(tables[...], gathered[:, :, at].reshape(n_ma * 2 * orders, wide_block))
        lane_cycle = iota((8, wide_block), 1) // (2 * vectors)
        begin = jnp.zeros((8, wide_block), I32)
        length = jnp.zeros((8, wide_block), I32)
        weight = jnp.zeros((8, wide_block), F32)
        for r in range(cycles_here):
            here = lane_cycle == r
            cycle = first + block * cycles_here + r
            begin = jnp.where(here, start_ref[cycle], begin)
            length = jnp.where(here, count_ref[cycle], length)
            weight = jnp.where(here, weight_ref[cycle], weight)
        away = iota(grid.shape, 0) - begin[:1]
        away = jnp.where(away < 0, away + longitudes, away)
        weighted = (grid * jnp.where(away < length[:1], weight[:1], 0.0)).astype(BF16)
        found = mm(back_table[...], weighted)
        for n in range(wide_block // LANES):
            both = found[:, n * LANES : (n + 1) * LANES]
            c, s = both[:orders], both[orders:]
            pair = [jnp.where(front, c, swap(s)), jnp.where(front, swap(c), s)]
            for e in range(2):
                cycle = block * cycles_here + 2 * n + e
                returned[rows_at(cycle, orders), :] = pair[e]
        return carry

    lax.fori_loop(0, columns // wide_block, transform, 0)
    here = returned[...]
    even = lax.rem(iota(here.shape, 1) // vectors, 2) == 0
    turned = jnp.concatenate([here, jnp.where(even, right(here), left(here))], axis=0).T
    turned = turned.astype(BF16)
    g_x = turned[:vectors]
    back_y = turned[vectors : 2 * vectors]
    g_y = turned[2 * vectors : 3 * vectors]
    back_x = turned[3 * vectors :]
    packed[vert, :, : 2 * terms] = g_x
    packed[vert, :, 2 * terms :] = g_y
    gather_start(0, packed)
    send_far(cuts[0], cuts[1])

    signs = sign.astype(BF16)
    adjoint = jnp.concatenate([g_x * signs, g_y, -back_y, -back_x * signs], axis=0)
    products = mm(adjoint, llm[0]) + mm(adjoint, llm[1]) + mm(adjoint, llm[2])
    part = [products[c * vectors : (c + 1) * vectors] for c in range(parts)]
    gram_x = part[0] * sign + swap(part[3] * -sign)
    gram_y = part[1] - swap(part[2])
    for n, (piece_x, piece_y) in enumerate(zip(split(gram_x, 3), split(gram_y, 3))):
        at = slice(n * vectors, (n + 1) * vectors)
        lhs[at, : 2 * terms] = piece_x
        lhs[at, 2 * terms :] = piece_y

    gather_wait(0, packed)
    everyone = packed[...].reshape(total, 4 * terms)
    found = mm_nt(lhs[...], everyone)
    found = [found[n * vectors : (n + 1) * vectors] for n in range(6)]
    row_a[...] = found[0] + found[1] + found[2]
    ma_start(1, row_a, land_a)
    land_a[ma] = row_a[...]
    row_b[...] = found[3] + found[4] + found[5]
    land_b[ma] = row_b[...]

    for i in range(n_vert):
        near_copy(i, 1 - place).wait_recv()
    wide = parts * vectors
    near_sums = jnp.zeros((wide, 2 * wide), F32)
    for i in range(n_vert):
        for e in range(share):
            here = mine[i, e].reshape(wide, degrees)
            both = jnp.concatenate([here, theirs[pair_at(i), e].reshape(wide, degrees)], axis=0)
            near_sums = near_sums + mm_nt(here, both)
    first_half, second_half = [
        sum(
            near_sums[c * vectors : (c + 1) * vectors, n * wide + c * vectors : n * wide + (c + 1) * vectors]
            for c in range(parts)
        )
        for n in range(2)
    ]
    near_sums = jnp.concatenate([first_half, second_half], axis=1)
    swapped = jnp.concatenate([second_half, first_half], axis=1)
    near_sums = jnp.where(place == 0, near_sums, swapped)
    row_e[...] = jnp.concatenate([near_sums[: vectors // 2], near_sums[vectors // 2 :]], axis=1)
    ma_start(4, row_e, land_e)
    land_e[ma] = row_e[...]

    ma_wait(1, row_a, land_a)
    sum_a[vert] = jnp.sum(land_a[...], axis=0)
    gather_start(1, sum_a)
    send_far(cuts[1], cuts[2])
    ma_start(2, row_b, land_b)
    ma_wait(4, row_e, land_e)
    sum_e[vert] = jnp.sum(land_e[...], axis=0)
    vert_start(4, sum_e.at[vert], sum_e)
    send_far(cuts[2], pieces)

    gather_wait(1, sum_a)
    inverse_count = 1.0 / (n_ma * orders * parts * degrees)
    work[:, :total] = sum_a[...].reshape(total, total) * inverse_count
    work[:, total:] = (iota((total, total), 0) == iota((total, total), 1)).astype(F32)

    def panel_step(p, carry):
        factor_panel(work, p)
        return carry

    panels = total // PANEL
    lax.fori_loop(0, panels // 2, panel_step, 0)

    ma_wait(2, row_b, land_b)
    sum_b[vert] = jnp.sum(land_b[...], axis=0)

    def far_wait(piece, carry):
        far_copy(piece, True).wait_recv()
        return carry

    lax.fori_loop(0, pieces, far_wait, 0)

    cross_sums = jnp.zeros((2 * wide, 2 * wide), F32)
    for e in range(share):
        here = [mine[half, e].reshape(wide, degrees), theirs[vert, e].reshape(wide, degrees)]
        there = far[:, e].reshape(half * wide, degrees)
        cross_sums = cross_sums + mm_nt(jnp.concatenate(here, axis=0), there)
    cross_sums = jnp.concatenate(
        [
            jnp.concatenate(
                [
                    sum(
                        cross_sums[
                            m * wide + c * vectors : m * wide + (c + 1) * vectors,
                            n * wide + c * vectors : n * wide + (c + 1) * vectors,
                        ]
                        for c in range(parts)
                    )
                    for n in range(2)
                ],
                axis=1,
            )
            for m in range(2)
        ],
        axis=0,
    )
    swapped = jnp.concatenate([cross_sums[vectors:], cross_sums[:vectors]], axis=0)
    cross_sums = jnp.where(place == 0, cross_sums, swapped)
    cross_sums = jnp.where(side == 0, cross_sums, cross_sums.T)
    size = half * vectors
    ab_own[...] = jnp.concatenate([cross_sums[: size // 2], cross_sums[size // 2 :]], axis=1)
    vert_start(3, ab_own, land_c)
    land_c[vert] = ab_own[...]

    vert_wait(4, sum_e.at[vert], sum_e)
    blocks = sum_e[...]
    size = half * vectors
    near_blocks = [
        jnp.concatenate([blocks[n][:, :size], blocks[n][:, size:]], axis=0) * inverse_count
        for n in range(n_vert)
    ]
    diagonals = [jnp.concatenate(near_blocks[n * half : (n + 1) * half], axis=0) for n in range(2)]
    unit = (iota((size, size), 0) == iota((size, size), 1)).astype(F32)
    corner[...] = jnp.concatenate([diagonals[0], unit], axis=1)

    def both_step(p, carry):
        factor_panel(work, panels // 2 + p)
        factor_panel(corner, p)
        return carry

    lax.fori_loop(0, panels // 2, both_step, 0)
    in_front = iota(corner.shape, 1) < size
    inverse = jnp.where(in_front, swap(corner[...]), 0.0)
    corner_ref[...] = jnp.concatenate([inverse[:, :size], diagonals[1]], axis=1)

    vert_wait(3, ab_own, land_c)
    ab_mid[...] = jnp.sum(land_c[...], axis=0)
    ma_start(3, ab_mid, land_d)
    land_d[ma] = ab_mid[...]
    vert_start(2, sum_b.at[vert], sum_b)

    mixing = work[rows_at(vert, vectors), total:].astype(BF16)
    spread = (iota((parts * vectors, vectors), 0) // parts == iota((parts * vectors, vectors), 1))
    mixing = mm(spread.astype(BF16), mixing).astype(BF16)
    mixed = mm(mixing, everyone)
    mixed_x, mixed_y = mixed[:, : 2 * terms], mixed[:, 2 * terms :]
    kind = lax.rem(iota(mixed_x.shape, 0), parts)
    sign = half_sign(mixed_x.shape, 1.0, -1.0)
    mixer = jnp.where(
        kind == 0, mixed_x * sign,
        jnp.where(kind == 1, mixed_y, jnp.where(kind == 2, -swap(mixed_y), -swap(mixed_x) * sign)),
    )
    pieces_of = split(mixer, 2)
    lane_order = modulo(iota(mixer.shape, 1), orders)

    def mix(s, carry):
        chosen = [jnp.where(lane_order == s, piece, jnp.zeros_like(piece)) for piece in pieces_of]
        mixed = mm(chosen[0], leg_ref[...]) + mm(chosen[1], leg_ref[...])
        basis_ref[:, s] = mixed.reshape(vectors, parts, degrees).astype(BF16)
        return carry

    lax.fori_loop(0, orders, mix, 0)

    vert_wait(2, sum_b.at[vert], sum_b)
    lower = (iota((size, total), 0) + size == iota((size, total), 1)).astype(F32)
    outer = jnp.concatenate([inverse, lower], axis=0)
    crossed = jnp.dot(
        outer, sum_b[...].reshape(total, total) * inverse_count,
        precision=HIGHEST, preferred_element_type=F32,
    )
    cross_ref[...] = lax.dot_general(
        crossed, outer, NT, precision=HIGHEST, preferred_element_type=F32
    )
    ma_wait(3, ab_mid, land_d)
    ab_ref[...] = jnp.sum(land_d[...], axis=0) * inverse_count

    for i in range(n_vert):
        near_copy(i, place).wait_send()

    def far_done(piece, carry):
        far_copy(piece).wait_send()
        return carry

    lax.fori_loop(0, pieces, far_done, 0)
    ma_done(0, message, gathered)
    gather_done(0, packed)
    ma_done(1, row_a, land_a)
    ma_done(2, row_b, land_b)
    gather_done(1, sum_a)
    vert_done(2, sum_b.at[vert], sum_b)
    ma_done(4, row_e, land_e)
    vert_done(4, sum_e.at[vert], sum_e)
    vert_done(3, ab_own, land_c)
    ma_done(3, ab_mid, land_d)


def step_terms(trial, legendre, order_slot, cycle_start, cycle_count, cycle_weight, n_ma, n_vert):
    vectors, orders, per, _ = trial.shape
    _, kinds, cycles, degrees = legendre.shape
    parts = per * LANES // degrees
    live = cycles // 4
    terms = live * orders
    total = n_vert * vectors
    half = n_vert // 2
    share = orders // n_vert
    longitudes = 2 * n_ma * orders
    pieces = half * share * parts
    columns = live * 2 * vectors
    grant = min(60, 16 + terms // 16) * MIB
    anywhere = pl.BlockSpec(memory_space=pltpu.HBM)
    return pl.pallas_call(
        functools.partial(step_kernel, n_ma, n_vert, live),
        out_shape=(
            jax.ShapeDtypeStruct((total, total), F32),
            jax.ShapeDtypeStruct((half * vectors, 2 * half * vectors), F32),
            jax.ShapeDtypeStruct((half * vectors // 2, 2 * half * vectors), F32),
            jax.ShapeDtypeStruct((vectors, orders, parts, degrees), BF16),
        ),
        in_specs=[anywhere] * 6,
        out_specs=[pl.BlockSpec(memory_space=VMEM)] * 4,
        scratch_shapes=[
            VMEM((2 * terms, degrees), BF16),
            VMEM((n_vert, vectors, share, per, LANES), BF16),
            VMEM(legendre.shape, BF16),
            VMEM((n_vert, share, parts, vectors, degrees), BF16),
            VMEM((n_vert, share, parts, vectors, degrees), BF16),
            VMEM((half, share, parts, vectors, degrees), BF16),
            VMEM((2 * orders, columns), BF16),
            VMEM((n_ma, 2 * orders, columns), BF16),
            VMEM((2 * terms, LANES), F32),
            VMEM((terms, LANES), F32),
            VMEM((n_vert, vectors, 4 * terms), BF16),
            VMEM((vectors, total), F32),
            VMEM((n_ma, vectors, total), F32),
            VMEM((n_vert, vectors, total), F32),
            VMEM((vectors, total), F32),
            VMEM((n_ma, vectors, total), F32),
            VMEM((n_vert, vectors, total), F32),
            VMEM((vectors // 2, 2 * half * vectors), F32),
            VMEM((n_ma, vectors // 2, 2 * half * vectors), F32),
            VMEM((n_vert, vectors // 2, 2 * half * vectors), F32),
            VMEM((half * vectors // 2, 2 * half * vectors), F32),
            VMEM((n_vert, half * vectors // 2, 2 * half * vectors), F32),
            VMEM((half * vectors // 2, 2 * half * vectors), F32),
            VMEM((n_ma, half * vectors // 2, 2 * half * vectors), F32),
            VMEM((total, 2 * total), F32),
            VMEM((half * vectors, 2 * half * vectors), F32),
            VMEM((6 * vectors, 4 * terms), BF16),
            VMEM((3, 2 * terms, 2 * terms), BF16),
            VMEM((longitudes, n_ma * 2 * orders), BF16),
            VMEM((2 * orders, longitudes), BF16),
            SMEM(order_slot.shape, I32),
            SMEM(cycle_start.shape, I32),
            SMEM(cycle_count.shape, I32),
            SMEM(cycle_weight.shape, F32),
            DMA((n_vert,)),
            DMA,
            DMA((4,)),
            DMA((n_vert,)),
            DMA((n_vert,)),
            DMA((pieces,)),
            DMA((pieces,)),
            DMA((5, n_ma)),
            DMA((5, n_ma)),
            DMA((5, n_vert)),
            DMA((5, n_vert)),
        ],
        compiler_params=pltpu.CompilerParams(
            collective_id=0, has_side_effects=True, vmem_limit_bytes=grant
        ),
        name="step_terms",
    )(trial, legendre, order_slot, cycle_start, cycle_count, cycle_weight)


def finish_kernel(cross_ref, corner_ref, ab_ref, staged_ref, basis_ref, ritz_ref, work, sem):
    total = ritz_ref.shape[0]
    size = total // 2
    out = pltpu.make_async_copy(staged_ref, basis_ref, sem)
    out.start()
    ab = ab_ref[...]
    ab = jnp.concatenate([ab[:, :size], ab[:, size:]], axis=0)
    inverse, diagonal = corner_ref[:, :size], corner_ref[:, size:]
    beside = jnp.dot(inverse, ab, precision=HIGHEST, preferred_element_type=F32)
    taken = fine(beside, beside, 0, 0)
    unit = (iota((size, size), 0) == iota((size, size), 1)).astype(F32)
    work[:, :total] = jnp.concatenate([diagonal - taken, jnp.zeros_like(unit)], axis=1)
    turned = lax.dot_general(
        ab, inverse, (((0,), (1,)), ((), ())), precision=HIGHEST, preferred_element_type=F32
    )
    work[:, total:] = jnp.concatenate([-turned, unit], axis=1)

    def step(p, carry):
        factor_panel(work, p)
        return carry

    lax.fori_loop(0, size // PANEL, step, 0)
    upper = (iota((size, total), 0) == iota((size, total), 1)).astype(F32)
    outer = jnp.concatenate([upper, work[:, total:]], axis=0)
    ritz_ref[...] = fine(fine(outer, cross_ref[...], 1, 0), outer, 1, 1)
    out.wait()


def finish(cross, corner, ab, staged):
    total = cross.shape[0]
    return pl.pallas_call(
        finish_kernel,
        out_shape=(
            jax.ShapeDtypeStruct(staged.shape, BF16),
            jax.ShapeDtypeStruct((total, total), F32),
        ),
        in_specs=[pl.BlockSpec(memory_space=VMEM)] * 4,
        out_specs=(pl.BlockSpec(memory_space=pl.ANY), pl.BlockSpec(memory_space=VMEM)),
        scratch_shapes=[VMEM((total // 2, 2 * total), F32), DMA],
        compiler_params=pltpu.CompilerParams(vmem_limit_bytes=8 * MIB),
        name="finish",
    )(cross, corner, ab, staged)


def shards(trial_block, legendre, order_slot, cycle_start, cycle_count, cycle_weight):
    n_ma = lax.axis_size("ma")
    n_vert = lax.axis_size("vert")
    vectors, orders, parts, degrees = trial_block.shape
    trial = trial_block.reshape(vectors, orders, parts, degrees // LANES, LANES)
    trial = trial.transpose(0, 1, 3, 2, 4).reshape(vectors, orders, parts * degrees // LANES, LANES)
    inputs = (trial, legendre, order_slot, cycle_start, cycle_count, cycle_weight)
    inputs = [pltpu.with_memory_space_constraint(x, pltpu.HBM) for x in inputs]
    return finish(*step_terms(*inputs, n_ma, n_vert))


def solution(mesh):
    in_specs = (P("vert", "ma", None, None), P("ma", None, None, None), P(), P(), P(), P())
    out_specs = (P("vert", "ma", None, None), P())
    return jax.shard_map(shards, mesh=mesh, in_specs=in_specs, out_specs=out_specs, check_vma=False)
```
